128 devices in a mesh: row: 16 (over y, x), col: 8 (over z, core).
Axes of the slice: x: 4, y: 4, z: 4, core: 2. Of those that a mesh axis runs over, the one named last changes fastest.
Arguments:
- species: float32 [2, 512, 512, 256], P(None, None, 'row', 'col'), may hold values from -6 to 6
- coupling: float32 [2, 2], replicated, may hold values from -4 to 4
- symbol_x: float32 [512], replicated, may hold values from 0.3 to 3
- symbol_y: float32 [512], replicated, may hold values from 0.3 to 3
- symbol_z: float32 [256], replicated, may hold values from 0.3 to 3
Outputs:
- modes: float32 [2, 512, 512, 256], P(None, 'row', 'col')
The draws below stay inside these ranges and needn't reach their ends.
All inputs are finite; a program needn't handle non-finite values.
Results may differ from the reference program's by a relative error of at most 0.000078.
Values sent between devices are 32-bit elements.
A program may use at most 128 MiB of HBM per device.

```python
import jax
import jax.numpy as jnp
from jax import lax

GRID_X = 512
GRID_Y = 512
GRID_Z = 256
FIELDS = 2


def block_scale(own_key, shape, cuts, low, top_value):
    level, own = 1.0, jax.random.fold_in(own_key, 6)
    for position, shards_of in cuts:
        draws = jnp.exp(jax.random.uniform(jax.random.fold_in(own, position), (shards_of,), jnp.float32, low / len(cuts), top_value / len(cuts)))
        level = level * jnp.repeat(draws, shape[position] // shards_of).reshape([-1 if axis == position else 1 for axis in range(len(shape))])
    return level


def scatter_about(key, extent, width, limit, shards=(), kind=jnp.bfloat16):
    values = width * jax.random.normal(key, extent, jnp.float32)
    if shards:
        values = values * block_scale(key, extent, shards, -0.22, 0.18)
    return jnp.clip(values, -limit, limit).astype(kind)


def setup_inputs(seed: int = 0) -> dict:
    seeds = jax.random.split(jax.random.key(seed), 6)
    species = scatter_about(seeds[0], (FIELDS, GRID_X, GRID_Y, GRID_Z), 1.0, 6.0, ((2, 16), (3, 8)), jnp.float32)
    coupling = scatter_about(seeds[1], (FIELDS, FIELDS), 0.7, 4.0, (), jnp.float32)
    symbol_x = jnp.clip(jax.random.uniform(seeds[2], (GRID_X,), jnp.float32, 0.3, 3.0), 0.3, 3.0)
    symbol_y = jnp.clip(jax.random.uniform(seeds[3], (GRID_Y,), jnp.float32, 0.3, 3.0), 0.3, 3.0)
    symbol_z = jnp.clip(jax.random.uniform(seeds[4], (GRID_Z,), jnp.float32, 0.3, 3.0), 0.3, 3.0)
    return {"species": species, "coupling": coupling, "symbol_x": symbol_x, "symbol_y": symbol_y, "symbol_z": symbol_z}


def mode_table(count):
    rank = jnp.arange(count)
    angle = (jnp.pi / (count + 1)) * (((rank[:, None] + 1) * (rank[None, :] + 1)) % (2 * count + 2)).astype(jnp.float32)
    return jnp.sin(angle) * (2.0 / (count + 1)) ** 0.5


def transform_dim(values, dim):
    moved = jnp.tensordot(values, mode_table(values.shape[dim]), axes=([dim], [0]), precision=lax.Precision.HIGHEST)
    return jnp.moveaxis(moved, -1, dim)


def reference(species, coupling, symbol_x, symbol_y, symbol_z):
    modes = species
    modes = transform_dim(modes, 1)
    modes = transform_dim(modes, 2)
    modes = transform_dim(modes, 3)
    symbol = symbol_x[:, None, None] + symbol_y[None, :, None] + symbol_z[None, None, :]
    weight_xyz = 1.0 / (1.0 + symbol)
    mixed_fields = jnp.einsum("ab,bxyz->axyz", coupling, modes, precision=lax.Precision.HIGHEST)
    modes = weight_xyz * modes + (1.0 - weight_xyz) * mixed_fields
    return modes
```

```python
import functools

import jax
import jax.numpy as jnp
import ml_dtypes
import numpy as np
from jax import lax
from jax.experimental import pallas as pl
from jax.experimental.pallas import tpu as pltpu
from jax.sharding import PartitionSpec as P

F32, BF16 = jnp.float32, jnp.bfloat16
MESH = pl.DeviceIdType.MESH
NX, NY, NZ, NF = 512, 512, 256, 2
RY, RX, CZ, CC = 4, 4, 4, 2
ROWS, COLS = RY * RX, CZ * CC
KX, KY = NX // ROWS, NY // COLS
YL, ZL = NY // ROWS, NZ // COLS
STEP = 8
PARTS = KX // STEP
CHUNKS = PARTS * NF
LAG_Y, LAG_Z = 2, 4
ROW_ORDER = (1, 4, 3, 12, 5, 15, 7, 13, 2, 8, 6, 9, 11, 14, 10)
COL_ORDER = (2, 6, 3, 7, 4, 5, 1)


def mode_table(count):
    rank = np.arange(1, count + 1)
    turns = np.outer(rank, rank) % (2 * count + 2)
    return np.sin(np.pi / (count + 1) * turns) * np.sqrt(2.0 / (count + 1))


def two_terms(table):
    high = table.astype(np.float32).astype(ml_dtypes.bfloat16)
    low = (table - high.astype(np.float64)).astype(np.float32).astype(ml_dtypes.bfloat16)
    return high, low


def tables():
    high, low = two_terms(mode_table(NX))
    pick = lambda t: t.reshape(ROWS, PARTS, STEP, NX).transpose(1, 0, 2, 3).reshape(PARTS, ROWS * STEP, NX)
    table_x = np.concatenate([pick(high), pick(low)], axis=1)
    high, low = two_terms(mode_table(NY))
    swap = lambda t: t.reshape(NY, ROWS, YL // 4, 4).transpose(0, 1, 3, 2).reshape(NY, NY)
    table_y = np.stack([swap(high), swap(low)])
    table_z = np.stack(two_terms(mode_table(NZ)))
    return table_x, table_y, table_z


def split(values):
    high = values.astype(BF16)
    return high, (values - high.astype(F32)).astype(BF16)


def dot(a, b, b_dim=0):
    return lax.dot_general(a, b, (((1,), (b_dim,)), ((), ())), preferred_element_type=F32)


def exchange_groups(values):
    lane = lax.broadcasted_iota(jnp.int32, values[0].shape, 1)
    low_half, even = lane < 64, lane % 64 < 32
    a, b, c, d = values
    a, c = jnp.where(low_half, a, pltpu.roll(c, 64, 1)), jnp.where(low_half, pltpu.roll(a, 64, 1), c)
    b, d = jnp.where(low_half, b, pltpu.roll(d, 64, 1)), jnp.where(low_half, pltpu.roll(b, 64, 1), d)
    a, b = jnp.where(even, a, pltpu.roll(b, 32, 1)), jnp.where(even, pltpu.roll(a, 96, 1), b)
    c, d = jnp.where(even, c, pltpu.roll(d, 32, 1)), jnp.where(even, pltpu.roll(c, 96, 1), d)
    return a, b, c, d


def kernel(
    coupling, sym_x, sym_y, sym_z, field, table_x, table_y, table_z, out,
    raw, high, low, tx, ty, tz, turn, row_out, row_in, col_out, col_in, base, first, result,
    load_sem, row_send, row_recv, col_send, col_recv, store_sem,
):
    row, col = lax.axis_index("row"), lax.axis_index("col")

    def row_peer(shift):
        return (row // RX + shift // RX) % RY * RX + (row + shift % RX) % RX

    def col_peer(shift):
        return (col // CC + shift // CC) % CZ * CC + (col + shift % CC) % CC

    loads = [
        pltpu.make_async_copy(field.at[0], raw.at[0], load_sem.at[0]),
        pltpu.make_async_copy(table_x, tx, load_sem.at[1]),
        pltpu.make_async_copy(field.at[1], raw.at[1], load_sem.at[2]),
        pltpu.make_async_copy(table_y, ty, load_sem.at[3]),
        pltpu.make_async_copy(table_z, tz, load_sem.at[4]),
    ]
    for load in loads:
        load.start()

    barrier = pltpu.get_barrier_semaphore()
    for shift in ROW_ORDER:
        pl.semaphore_signal(barrier, inc=1, device_id=(row_peer(shift), col), device_id_type=MESH)
    for shift in COL_ORDER:
        pl.semaphore_signal(barrier, inc=1, device_id=(row, col_peer(shift)), device_id_type=MESH)

    for block in range(NY // 128):
        lanes = jnp.broadcast_to(sym_y[:, block * 128:(block + 1) * 128], (128, 128))
        turn[0, 0:64] = jnp.transpose(lanes)[0:64]
        turn[1, 0:64] = jnp.transpose(lanes)[64:128]

        @pl.when(col // 2 == block)
        def _():
            mine = turn[col % 2]
            base[...] = 1.0 + jnp.concatenate([mine, mine], axis=1) + sym_z[...]

    def split_field(a):
        def body(n, carry):
            rows = pl.ds(pl.multiple_of(n * 128, 128), 128)
            high[a, rows, :], low[a, rows, :] = split(raw[a, rows, :])
            return carry
        lax.fori_loop(0, YL * ZL // 128, body, 0)

    def x_step(i):
        a, q = i % NF, i // NF

        def body(n, carry):
            rows = pl.ds(pl.multiple_of(n * 256, 256), 256)
            both = dot(tx[q], high[a, rows, :], 1)
            values = both[:128] + both[128:] + dot(tx[q, 0:128], low[a, rows, :], 1)
            for r in range(ROWS):
                for half in range(2):
                    turn[r, pl.ds(n * 2 + half, 8, stride=8), :] = values[r * 8:(r + 1) * 8, half * 128:(half + 1) * 128]
            return carry
        lax.fori_loop(0, YL * ZL // 256, body, 0)

        for r in range(0, ROWS, 4):
            for kb in range(2):
                parts = [turn[r:r + 4, (kb * 4 + k) * 8:(kb * 4 + k + 1) * 8, :].reshape(32, 128) for k in range(4)]
                for g, part in enumerate(exchange_groups(parts)):
                    row_out[i, r:r + 4, kb, g * 8:(g + 1) * 8, :] = part.reshape(4, 8, 128)

        for shift in ROW_ORDER:
            peer = row_peer(shift)
            pltpu.make_async_remote_copy(
                src_ref=row_out.at[i, peer], dst_ref=row_in.at[i, row], send_sem=row_send, recv_sem=row_recv.at[i],
                device_id=(peer, col), device_id_type=MESH,
            ).start()
        pltpu.make_async_copy(row_out.at[i, row], row_in.at[i, row], row_recv.at[i]).start()

    def y_step(i):
        pltpu.make_async_copy(row_in.at[i], row_in.at[i], row_recv.at[i]).wait()
        lines = jnp.concatenate([row_in[i, :, kb].reshape(NY, 128) for kb in range(2)], axis=1)
        lines_high, lines_low = split(lines)
        values = dot(ty[0], lines_high) + dot(ty[1], lines_high) + dot(ty[0], lines_low)
        for kb in range(2):
            col_out[i, :, kb] = values[:, kb * 128:(kb + 1) * 128].reshape(COLS, KY, 128)
        for shift in COL_ORDER:
            peer = col_peer(shift)
            pltpu.make_async_remote_copy(
                src_ref=col_out.at[i, peer], dst_ref=col_in.at[i, col], send_sem=col_send, recv_sem=col_recv.at[i],
                device_id=(row, peer), device_id_type=MESH,
            ).start()
        pltpu.make_async_copy(col_out.at[i, col], col_in.at[i, col], col_recv.at[i]).start()

    def z_step(i):
        a, q = i % NF, i // NF
        pltpu.make_async_copy(col_in.at[i], col_in.at[i], col_recv.at[i]).wait()

        for kb in range(2):
            halves = [exchange_groups([col_in[i, h * 4 + j, kb] for j in range(4)]) for h in range(2)]
            for k in range(4):
                lines_high, lines_low = split(jnp.concatenate([halves[0][k], halves[1][k]], axis=1))
                values = dot(lines_high, tz[0]) + dot(lines_high, tz[1]) + dot(lines_low, tz[0])
                x = kb * 4 + k

                @pl.when(a == 0)
                def _():
                    first[x] = values

                @pl.when(a == 1)
                def _():
                    other = first[x]
                    weight = 1.0 / (base[...] + sym_x[row * KX + q * STEP + x])
                    rest = 1.0 - weight
                    result[0, q * STEP + x] = weight * other + rest * (coupling[0, 0] * other + coupling[0, 1] * values)
                    result[1, q * STEP + x] = weight * values + rest * (coupling[1, 0] * other + coupling[1, 1] * values)

        @pl.when(a == 1)
        def _():
            part = pl.ds(pl.multiple_of(q * STEP, STEP), STEP)
            pltpu.make_async_copy(result.at[:, part], out.at[:, part], store_sem).start()

    loads[0].wait()
    split_field(0)
    loads[1].wait()
    pl.semaphore_wait(barrier, ROWS + COLS - 2)

    def loop(t, carry):
        @pl.when(t == 1)
        def _():
            loads[2].wait()
            split_field(1)

        @pl.when(t < CHUNKS)
        def _():
            x_step(t)

        @pl.when(t == LAG_Y)
        def _():
            loads[3].wait()

        @pl.when(jnp.logical_and(t >= LAG_Y, t < CHUNKS + LAG_Y))
        def _():
            y_step(t - LAG_Y)

        @pl.when(t == LAG_Z)
        def _():
            loads[4].wait()

        @pl.when(t >= LAG_Z)
        def _():
            z_step(t - LAG_Z)
        return carry

    lax.fori_loop(0, CHUNKS + LAG_Z, loop, 0)
    sent = row_out.at[:, pl.ds(0, ROWS - 1)]
    pltpu.make_async_copy(sent, sent, row_send).wait()
    sent = col_out.at[:, pl.ds(0, COLS - 1)]
    pltpu.make_async_copy(sent, sent, col_send).wait()
    pltpu.make_async_copy(result, out, store_sem).wait()


def local(species, coupling, symbol_x, symbol_y, symbol_z):
    field = jnp.transpose(species, (0, 2, 3, 1)).reshape(NF, YL * ZL, NX)
    smem, vmem, far = (pl.BlockSpec(memory_space=m) for m in (pltpu.SMEM, pltpu.VMEM, pl.ANY))
    return pl.pallas_call(
        kernel,
        out_shape=jax.ShapeDtypeStruct((NF, KX, KY, NZ), F32),
        in_specs=[smem, smem, vmem, vmem, far, far, far, far],
        out_specs=far,
        scratch_shapes=[
            pltpu.VMEM((NF, YL * ZL, NX), F32),
            pltpu.VMEM((NF, YL * ZL, NX), BF16),
            pltpu.VMEM((NF, YL * ZL, NX), BF16),
            pltpu.VMEM((PARTS, 2 * ROWS * STEP, NX), BF16),
            pltpu.VMEM((2, NY, NY), BF16),
            pltpu.VMEM((2, NZ, NZ), BF16),
            pltpu.VMEM((ROWS, 64, 128), F32),
            pltpu.VMEM((CHUNKS, ROWS, 2, YL, 128), F32),
            pltpu.VMEM((CHUNKS, ROWS, 2, YL, 128), F32),
            pltpu.VMEM((CHUNKS, COLS, 2, KY, 128), F32),
            pltpu.VMEM((CHUNKS, COLS, 2, KY, 128), F32),
            pltpu.VMEM((KY, NZ), F32),
            pltpu.VMEM((STEP, KY, NZ), F32),
            pltpu.VMEM((NF, KX, KY, NZ), F32),
            pltpu.SemaphoreType.DMA((5,)),
            pltpu.SemaphoreType.DMA,
            pltpu.SemaphoreType.DMA((CHUNKS,)),
            pltpu.SemaphoreType.DMA,
            pltpu.SemaphoreType.DMA((CHUNKS,)),
            pltpu.SemaphoreType.DMA,
        ],
        compiler_params=pltpu.CompilerParams(collective_id=1, has_side_effects=True, vmem_limit_bytes=52 << 20),
        name="sine_modes",
    )(coupling, symbol_x, symbol_y.reshape(1, NY), symbol_z.reshape(1, NZ), field, *map(jnp.asarray, tables()))


def solution(mesh):
    return jax.shard_map(
        local,
        mesh=mesh,
        in_specs=(P(None, None, "row", "col"), P(), P(), P(), P()),
        out_specs=P(None, "row", "col", None),
        check_vma=False,
    )
```

```python
import functools

import jax
import jax.numpy as jnp
import ml_dtypes
import numpy as np
from jax import lax
from jax.experimental import pallas as pl
from jax.experimental.pallas import tpu as pltpu
from jax.sharding import PartitionSpec as P

F32, BF16 = jnp.float32, jnp.bfloat16
MESH = pl.DeviceIdType.MESH
NX, NY, NZ, NF = 512, 512, 256, 2
RY, RX, CZ, CC = 4, 4, 4, 2
ROWS, COLS = RY * RX, CZ * CC
KX, KY = NX // ROWS, NY // COLS
YL, ZL = NY // ROWS, NZ // COLS
STEP = 8
PARTS = KX // STEP
CHUNKS = PARTS * NF
LAG_Y, LAG_Z = 2, 4
ROW_ORDER = (1, 4, 3, 12, 5, 15, 7, 13, 2, 8, 6, 9, 11, 14, 10)
COL_ORDER = (2, 6, 3, 7, 4, 5, 1)


def mode_table(count):
    rank = np.arange(1, count + 1)
    turns = np.outer(rank, rank) % (2 * count + 2)
    return np.sin(np.pi / (count + 1) * turns) * np.sqrt(2.0 / (count + 1))


def two_terms(table):
    high = table.astype(np.float32).astype(ml_dtypes.bfloat16)
    low = (table - high.astype(np.float64)).astype(np.float32).astype(ml_dtypes.bfloat16)
    return high, low


def tables():
    high, low = two_terms(mode_table(NX))
    pick = lambda t: t.reshape(ROWS, PARTS, STEP, NX).transpose(1, 0, 2, 3).reshape(PARTS, ROWS * STEP, NX)
    table_x = np.concatenate([pick(high), pick(low)], axis=1)
    high, low = two_terms(mode_table(NY))
    swap = lambda t: t.reshape(NY, ROWS, YL // 4, 4).transpose(0, 1, 3, 2).reshape(NY, NY)
    table_y = np.stack([swap(high), swap(low)])
    table_z = np.stack(two_terms(mode_table(NZ)))
    return table_x, table_y, table_z


def split(values):
    high = values.astype(BF16)
    return high, (values - high.astype(F32)).astype(BF16)


def dot(a, b, b_dim=0):
    return lax.dot_general(a, b, (((1,), (b_dim,)), ((), ())), preferred_element_type=F32)


def exchange_groups(values):
    lane = lax.broadcasted_iota(jnp.int32, values[0].shape, 1)
    low_half, even = lane < 64, lane % 64 < 32
    a, b, c, d = values
    a, c = jnp.where(low_half, a, pltpu.roll(c, 64, 1)), jnp.where(low_half, pltpu.roll(a, 64, 1), c)
    b, d = jnp.where(low_half, b, pltpu.roll(d, 64, 1)), jnp.where(low_half, pltpu.roll(b, 64, 1), d)
    a, b = jnp.where(even, a, pltpu.roll(b, 32, 1)), jnp.where(even, pltpu.roll(a, 96, 1), b)
    c, d = jnp.where(even, c, pltpu.roll(d, 32, 1)), jnp.where(even, pltpu.roll(c, 96, 1), d)
    return a, b, c, d


def kernel(
    coupling_far, sym_x_far, sym_y_far, sym_z_far, field, table_x, table_y, table_z, result,
    coupling, sym_x, sym_y, sym_z, raw, high, low, tx, ty, tz, turn, row_out, row_in, col_out, col_in, base, first,
    load_sem, row_send, row_recv, col_send, col_recv,
):
    row, col = lax.axis_index("row"), lax.axis_index("col")

    def row_peer(shift):
        return (row // RX + shift // RX) % RY * RX + (row + shift % RX) % RX

    def col_peer(shift):
        return (col // CC + shift // CC) % CZ * CC + (col + shift % CC) % CC

    loads = [
        pltpu.make_async_copy(field.at[0], raw.at[0], load_sem.at[0]),
        pltpu.make_async_copy(table_x, tx, load_sem.at[1]),
        pltpu.make_async_copy(field.at[1], raw.at[1], load_sem.at[2]),
        pltpu.make_async_copy(table_y, ty, load_sem.at[3]),
        pltpu.make_async_copy(table_z, tz, load_sem.at[4]),
        pltpu.make_async_copy(sym_y_far, sym_y, load_sem.at[5]),
        pltpu.make_async_copy(sym_z_far, sym_z, load_sem.at[6]),
        pltpu.make_async_copy(sym_x_far, sym_x, load_sem.at[7]),
        pltpu.make_async_copy(coupling_far, coupling, load_sem.at[8]),
    ]
    for load in loads:
        load.start()

    barrier = pltpu.get_barrier_semaphore()
    for shift in ROW_ORDER:
        pl.semaphore_signal(barrier, inc=1, device_id=(row_peer(shift), col), device_id_type=MESH)
    for shift in COL_ORDER:
        pl.semaphore_signal(barrier, inc=1, device_id=(row, col_peer(shift)), device_id_type=MESH)

    def split_field(a):
        def body(n, carry):
            rows = pl.ds(pl.multiple_of(n * 128, 128), 128)
            high[a, rows, :], low[a, rows, :] = split(raw[a, rows, :])
            return carry
        lax.fori_loop(0, YL * ZL // 128, body, 0)

    def make_base():
        for load in loads[5:]:
            load.wait()
        for block in range(NY // 128):
            lanes = jnp.transpose(jnp.broadcast_to(sym_y[:, block * 128:(block + 1) * 128], (128, 128)))

            @pl.when(col // 2 == block)
            def _():
                mine = jnp.where(col % 2 == 0, lanes[0:64], lanes[64:128])
                base[...] = 1.0 + jnp.concatenate([mine, mine], axis=1) + sym_z[...]

    def x_step(i):
        a, q = i % NF, i // NF

        def body(n, carry):
            rows = pl.ds(pl.multiple_of(n * 256, 256), 256)
            both = dot(tx[q], high[a, rows, :], 1)
            values = both[:128] + both[128:] + dot(tx[q, 0:128], low[a, rows, :], 1)
            for r in range(ROWS):
                for half in range(2):
                    turn[r, pl.ds(n * 2 + half, 8, stride=8), :] = values[r * 8:(r + 1) * 8, half * 128:(half + 1) * 128]
            return carry
        lax.fori_loop(0, YL * ZL // 256, body, 0)

        for r in range(0, ROWS, 4):
            for kb in range(2):
                parts = [turn[r:r + 4, (kb * 4 + k) * 8:(kb * 4 + k + 1) * 8, :].reshape(32, 128) for k in range(4)]
                for g, part in enumerate(exchange_groups(parts)):
                    row_out[i, r:r + 4, kb, g * 8:(g + 1) * 8, :] = part.reshape(4, 8, 128)

        for shift in ROW_ORDER:
            peer = row_peer(shift)
            pltpu.make_async_remote_copy(
                src_ref=row_out.at[i, peer], dst_ref=row_in.at[i, row], send_sem=row_send, recv_sem=row_recv.at[i],
                device_id=(peer, col), device_id_type=MESH,
            ).start()
        pltpu.make_async_copy(row_out.at[i, row], row_in.at[i, row], row_recv.at[i]).start()

    def y_step(i):
        pltpu.make_async_copy(row_in.at[i], row_in.at[i], row_recv.at[i]).wait()
        lines = jnp.concatenate([row_in[i, :, kb].reshape(NY, 128) for kb in range(2)], axis=1)
        lines_high, lines_low = split(lines)
        values = dot(ty[0], lines_high) + dot(ty[1], lines_high) + dot(ty[0], lines_low)
        for kb in range(2):
            col_out[i, :, kb] = values[:, kb * 128:(kb + 1) * 128].reshape(COLS, KY, 128)
        for shift in COL_ORDER:
            peer = col_peer(shift)
            pltpu.make_async_remote_copy(
                src_ref=col_out.at[i, peer], dst_ref=col_in.at[i, col], send_sem=col_send, recv_sem=col_recv.at[i],
                device_id=(row, peer), device_id_type=MESH,
            ).start()
        pltpu.make_async_copy(col_out.at[i, col], col_in.at[i, col], col_recv.at[i]).start()

    def z_step(i):
        a, q = i % NF, i // NF
        pltpu.make_async_copy(col_in.at[i], col_in.at[i], col_recv.at[i]).wait()

        for kb in range(2):
            halves = [exchange_groups([col_in[i, h * 4 + j, kb] for j in range(4)]) for h in range(2)]
            for k in range(4):
                lines_high, lines_low = split(jnp.concatenate([halves[0][k], halves[1][k]], axis=1))
                values = dot(lines_high, tz[0]) + dot(lines_high, tz[1]) + dot(lines_low, tz[0])
                x = kb * 4 + k

                @pl.when(a == 0)
                def _():
                    first[x] = values

                @pl.when(a == 1)
                def _():
                    other = first[x]
                    weight = 1.0 / (base[...] + sym_x[row * KX + q * STEP + x])
                    rest = 1.0 - weight
                    result[0, q * STEP + x] = weight * other + rest * (coupling[0, 0] * other + coupling[0, 1] * values)
                    result[1, q * STEP + x] = weight * values + rest * (coupling[1, 0] * other + coupling[1, 1] * values)

    loads[0].wait()
    split_field(0)
    loads[1].wait()
    pl.semaphore_wait(barrier, ROWS + COLS - 2)

    def loop(t, carry):
        @pl.when(t == 1)
        def _():
            loads[2].wait()
            split_field(1)

        @pl.when(t < CHUNKS)
        def _():
            x_step(t)

        @pl.when(t == LAG_Y)
        def _():
            loads[3].wait()

        @pl.when(jnp.logical_and(t >= LAG_Y, t < CHUNKS + LAG_Y))
        def _():
            y_step(t - LAG_Y)

        @pl.when(t == LAG_Z)
        def _():
            loads[4].wait()
            make_base()

        @pl.when(t >= LAG_Z)
        def _():
            z_step(t - LAG_Z)
        return carry

    lax.fori_loop(0, CHUNKS + LAG_Z, loop, 0)
    sent = row_out.at[:, pl.ds(0, ROWS - 1)]
    pltpu.make_async_copy(sent, sent, row_send).wait()
    sent = col_out.at[:, pl.ds(0, COLS - 1)]
    pltpu.make_async_copy(sent, sent, col_send).wait()


def local(species, coupling, symbol_x, symbol_y, symbol_z):
    field = jnp.transpose(species, (0, 2, 3, 1)).reshape(NF, YL * ZL, NX)
    operands = (coupling, symbol_x, symbol_y.reshape(1, NY), symbol_z.reshape(1, NZ), field, *map(jnp.asarray, tables()))
    far = pl.BlockSpec(memory_space=pltpu.HBM)
    return pl.pallas_call(
        kernel,
        out_shape=pltpu.VMEM((NF, KX, KY, NZ), F32),
        in_specs=[far] * 8,
        out_specs=pl.BlockSpec(memory_space=pltpu.VMEM),
        scratch_shapes=[
            pltpu.SMEM((NF, NF), F32),
            pltpu.SMEM((NX,), F32),
            pltpu.VMEM((1, NY), F32),
            pltpu.VMEM((1, NZ), F32),
            pltpu.VMEM((NF, YL * ZL, NX), F32),
            pltpu.VMEM((NF, YL * ZL, NX), BF16),
            pltpu.VMEM((NF, YL * ZL, NX), BF16),
            pltpu.VMEM((PARTS, 2 * ROWS * STEP, NX), BF16),
            pltpu.VMEM((2, NY, NY), BF16),
            pltpu.VMEM((2, NZ, NZ), BF16),
            pltpu.VMEM((ROWS, 64, 128), F32),
            pltpu.VMEM((CHUNKS, ROWS, 2, YL, 128), F32),
            pltpu.VMEM((CHUNKS, ROWS, 2, YL, 128), F32),
            pltpu.VMEM((CHUNKS, COLS, 2, KY, 128), F32),
            pltpu.VMEM((CHUNKS, COLS, 2, KY, 128), F32),
            pltpu.VMEM((KY, NZ), F32),
            pltpu.VMEM((STEP, KY, NZ), F32),
            pltpu.SemaphoreType.DMA((9,)),
            pltpu.SemaphoreType.DMA,
            pltpu.SemaphoreType.DMA((CHUNKS,)),
            pltpu.SemaphoreType.DMA,
            pltpu.SemaphoreType.DMA((CHUNKS,)),
        ],
        compiler_params=pltpu.CompilerParams(collective_id=1, has_side_effects=True, vmem_limit_bytes=40 << 20),
        name="sine_modes",
    )(*(pltpu.with_memory_space_constraint(operand, pltpu.HBM) for operand in operands))


def solution(mesh):
    return jax.shard_map(
        local,
        mesh=mesh,
        in_specs=(P(None, None, "row", "col"), P(), P(), P(), P()),
        out_specs=P(None, "row", "col", None),
        check_vma=False,
    )
```

```python
import functools

import jax
import jax.numpy as jnp
import ml_dtypes
import numpy as np
from jax import lax
from jax.experimental import pallas as pl
from jax.experimental.pallas import tpu as pltpu
from jax.sharding import PartitionSpec as P

F32, BF16 = jnp.float32, jnp.bfloat16
MESH = pl.DeviceIdType.MESH
NX, NY, NZ, NF = 512, 512, 256, 2
RY, RX, CZ, CC = 4, 4, 4, 2
ROWS, COLS = RY * RX, CZ * CC
KX, KY = NX // ROWS, NY // COLS
YL, ZL = NY // ROWS, NZ // COLS
STEP = 8
PARTS = KX // STEP
CHUNKS = PARTS * NF
LAG_Z = 2
ROW_ORDER = (1, 4, 3, 12, 5, 15, 7, 13, 2, 8, 6, 9, 11, 14, 10)
COL_ORDER = (2, 6, 3, 7, 4, 5, 1)


def mode_table(count):
    rank = np.arange(1, count + 1)
    turns = np.outer(rank, rank) % (2 * count + 2)
    return np.sin(np.pi / (count + 1) * turns) * np.sqrt(2.0 / (count + 1))


def two_terms(table):
    high = table.astype(np.float32).astype(ml_dtypes.bfloat16)
    low = (table - high.astype(np.float64)).astype(np.float32).astype(ml_dtypes.bfloat16)
    return high, low


def tables():
    high, low = two_terms(mode_table(NX))
    pick = lambda t: t.reshape(NX, ROWS, PARTS // 2, 2, STEP).transpose(2, 0, 3, 1, 4).reshape(PARTS // 2, NX, 2 * ROWS * STEP)
    table_x = np.stack([pick(high), pick(low)], axis=1)
    high, low = two_terms(mode_table(NY))
    swap = lambda t: t.reshape(NY // 128, 128, ROWS, YL // 4, 4).transpose(0, 1, 2, 4, 3).reshape(NY // 128, 128, NY)
    table_y = np.concatenate([swap(high), swap(low)], axis=1)
    table_z = np.stack(two_terms(mode_table(NZ)))
    return table_x, table_y, table_z


def split(values):
    high = values.astype(BF16)
    return high, (values - high.astype(F32)).astype(BF16)


def dot(a, b, b_dim=0):
    return lax.dot_general(a, b, (((1,), (b_dim,)), ((), ())), preferred_element_type=F32)


def exchange_groups(values):
    lane = lax.broadcasted_iota(jnp.int32, values[0].shape, 1)
    low_half, even = lane < 64, lane % 64 < 32
    a, b, c, d = values
    a, c = jnp.where(low_half, a, pltpu.roll(c, 64, 1)), jnp.where(low_half, pltpu.roll(a, 64, 1), c)
    b, d = jnp.where(low_half, b, pltpu.roll(d, 64, 1)), jnp.where(low_half, pltpu.roll(b, 64, 1), d)
    a, b = jnp.where(even, a, pltpu.roll(b, 32, 1)), jnp.where(even, pltpu.roll(a, 96, 1), b)
    c, d = jnp.where(even, c, pltpu.roll(d, 32, 1)), jnp.where(even, pltpu.roll(c, 96, 1), d)
    return a, b, c, d


def kernel(
    coupling_far, sym_x_far, sym_y_far, sym_z_far, field, table_x, table_y, table_z, result,
    coupling, sym_x, sym_y, sym_z, raw, tx, ty, tz, turn, row_out, row_in, col_out, col_in, base,
    load_sem, row_send, row_recv, col_send, col_recv,
):
    row, col = lax.axis_index("row"), lax.axis_index("col")
    row_peers = [(row // RX + s // RX) % RY * RX + (row + s % RX) % RX for s in ROW_ORDER]
    col_peers = [(col // CC + s // CC) % CZ * CC + (col + s % CC) % CC for s in COL_ORDER]
    last = CHUNKS - 1

    pairs = [(field.at[0], raw.at[0]), (table_x.at[0], tx.at[0]), (field.at[1], raw.at[1]), (table_x.at[1], tx.at[1])]
    pairs += [(table_y, ty), (table_z, tz), (sym_y_far, sym_y), (sym_z_far, sym_z), (sym_x_far, sym_x), (coupling_far, coupling)]
    loads = [pltpu.make_async_copy(src, dst, load_sem.at[n]) for n, (src, dst) in enumerate(pairs)]
    for load in loads:
        load.start()

    barrier = pltpu.get_barrier_semaphore()
    for peer in row_peers:
        pl.semaphore_signal(barrier, inc=1, device_id=(peer, col), device_id_type=MESH)
    for peer in col_peers:
        pl.semaphore_signal(barrier, inc=1, device_id=(row, peer), device_id_type=MESH)

    def wait_bytes(ref, sem):
        pltpu.make_async_copy(ref, ref, sem).wait()

    def make_base():
        for block in range(NY // 128):
            lanes = jnp.transpose(jnp.broadcast_to(sym_y[:, block * 128:(block + 1) * 128], (128, 128)))

            @pl.when(col // 2 == block)
            def _():
                mine = jnp.where(col % 2 == 0, lanes[0:64], lanes[64:128])
                base[...] = 1.0 + jnp.concatenate([mine, mine], axis=1) + sym_z[...]

    def row_exchange(i, kbs, sem):
        for peer in row_peers:
            pltpu.make_async_remote_copy(
                src_ref=row_out.at[i, peer, *kbs], dst_ref=row_in.at[i, row, *kbs], send_sem=row_send, recv_sem=sem,
                device_id=(peer, col), device_id_type=MESH,
            ).start()
        pltpu.make_async_copy(row_out.at[i, row, *kbs], row_in.at[i, row, *kbs], sem).start()

    def col_exchange(i, kbs, sem):
        for peer in col_peers:
            pltpu.make_async_remote_copy(
                src_ref=col_out.at[i, peer, *kbs], dst_ref=col_in.at[i, col, *kbs], send_sem=col_send, recv_sem=sem,
                device_id=(row, peer), device_id_type=MESH,
            ).start()
        pltpu.make_async_copy(col_out.at[i, col, *kbs], col_in.at[i, col, *kbs], sem).start()

    def x_step(u):
        h, a = u // 2, u % 2
        for n, when in enumerate((0, 0, 1, 2)):
            pl.when(u == when)(loads[n].wait)

        def lines(n, carry):
            rows = pl.ds(pl.multiple_of(n * 128, 128), 128)
            high, low = split(raw[a, rows, :])
            both = dot(jnp.concatenate([high, low], axis=0), tx[h, 0])
            values = both[:128] + both[128:] + dot(high, tx[h, 1])
            for b in range(2):
                flipped = jnp.transpose(values[:, b * 128:(b + 1) * 128])
                for r in range(ROWS):
                    turn[b, r, pl.ds(n, 8, stride=8), :] = flipped[r * 8:(r + 1) * 8]
            return carry
        lax.fori_loop(0, YL // 4, lines, 0, unroll=2)

        for b in range(2):
            i = 2 * u + b
            for kb in range(2):
                for r in range(0, ROWS, 4):
                    parts = [turn[b, r:r + 4, (kb * 4 + k) * 8:(kb * 4 + k + 1) * 8, :].reshape(32, 128) for k in range(4)]
                    for g, part in enumerate(exchange_groups(parts)):
                        row_out[i, r:r + 4, kb, g * 8:(g + 1) * 8, :] = part.reshape(4, 8, 128)
            if b == 0:
                pl.when(u == 0)(lambda: pl.semaphore_wait(barrier, ROWS + COLS - 2))
            ends = (u == 0) if b == 0 else (u == CHUNKS // 2 - 1)

            @pl.when(ends)
            def _():
                row_exchange(i, (0,), row_recv.at[i, 0])
                row_exchange(i, (1,), row_recv.at[i, 1])

            @pl.when(jnp.logical_not(ends))
            def _():
                row_exchange(i, (), row_recv.at[i, 0])

    def y_step(i, kb, count):
        kbs = pl.ds(kb, count)
        wait_bytes(row_in.at[i, :, kbs], row_recv.at[i, kb])
        lines = jnp.concatenate([row_in[i, :, kb + k].reshape(NY, 128) for k in range(count)], axis=1)
        high, low = split(lines)
        for m in range(NY // 128):
            both = dot(ty[m], high)
            values = both[:128] + both[128:] + dot(ty[m, 0:128], low)
            for k in range(count):
                col_out[i, 2 * m:2 * m + 2, kb + k] = values[:, k * 128:(k + 1) * 128].reshape(2, KY, 128)
        col_exchange(i, (kb,) if count == 1 else (), col_recv.at[i, kb])

    def z_wait(i, kb, count):
        wait_bytes(col_in.at[i, :, pl.ds(kb, count)], col_recv.at[i, kb])

    def z_step(i, kb, count):
        a, first_x = i // 2 % 2, (i // 4 * 2 + i % 2) * STEP + kb * 4
        for k in range(count):
            halves = [exchange_groups([col_in[i, g * 4 + j, kb + k] for j in range(4)]) for g in range(2)]
            for pair in range(2):
                lines = [jnp.concatenate([halves[0][2 * pair + e], halves[1][2 * pair + e]], axis=1) for e in range(2)]
                high, low = split(jnp.concatenate(lines, axis=0))
                both = dot(jnp.concatenate([high, low], axis=0), tz[0])
                values = both[:128] + both[128:] + dot(high, tz[1])
                x = first_x + k * 4 + 2 * pair
                result[a, pl.ds(x, 2)] = values.reshape(2, KY, NZ)

        @pl.when(a == 1)
        def _():
            def mix(n, carry):
                x = first_x + n
                one, two = result[0, x], result[1, x]
                weight = 1.0 / (base[...] + sym_x[row * KX + x])
                rest = 1.0 - weight
                result[0, x] = weight * one + rest * (coupling[0, 0] * one + coupling[0, 1] * two)
                result[1, x] = weight * two + rest * (coupling[1, 0] * one + coupling[1, 1] * two)
                return carry
            lax.fori_loop(0, 4 * count, mix, 0)

    def halves(step):
        def body(kb, carry):
            step(kb)
            return carry
        lax.fori_loop(0, 2, body, 0)

    def middle(i, carry):
        pl.when(jnp.logical_or(i == 1, i == 3))(lambda: x_step((i + 3) // 2))
        y_step(i, 0, 2)

        @pl.when(i == 2)
        def _():
            z_wait(0, 0, 1)
            z_wait(0, 1, 1)

        @pl.when(i > 2)
        def _():
            z_wait(i - LAG_Z, 0, 2)

        @pl.when(i >= 2)
        def _():
            z_step(i - LAG_Z, 0, 2)
        return carry

    halves(x_step)
    for load in loads[4:]:
        load.wait()
    make_base()
    halves(lambda kb: y_step(0, kb, 1))
    lax.fori_loop(1, last, middle, 0)

    def later(i, carry):
        pl.when(i == last - 1)(lambda: halves(lambda kb: y_step(last, kb, 1)))
        z_wait(i, 0, 2)
        z_step(i, 0, 2)
        return carry
    lax.fori_loop(last - 2, last, later, 0)

    def final(kb):
        z_wait(last, kb, 1)
        z_step(last, kb, 1)
    halves(final)
    wait_bytes(row_out.at[:, pl.ds(0, ROWS - 1)], row_send)
    wait_bytes(col_out.at[:, pl.ds(0, COLS - 1)], col_send)


def local(species, coupling, symbol_x, symbol_y, symbol_z):
    field = jnp.transpose(species, (0, 2, 3, 1)).reshape(NF, YL * ZL, NX)
    operands = (coupling, symbol_x, symbol_y.reshape(1, NY), symbol_z.reshape(1, NZ), field, *map(jnp.asarray, tables()))
    far = pl.BlockSpec(memory_space=pltpu.HBM)
    return pl.pallas_call(
        kernel,
        out_shape=pltpu.VMEM((NF, KX, KY, NZ), F32),
        in_specs=[far] * 8,
        out_specs=pl.BlockSpec(memory_space=pltpu.VMEM),
        scratch_shapes=[
            pltpu.SMEM((NF, NF), F32),
            pltpu.SMEM((NX,), F32),
            pltpu.VMEM((1, NY), F32),
            pltpu.VMEM((1, NZ), F32),
            pltpu.VMEM((NF, YL * ZL, NX), F32),
            pltpu.VMEM((PARTS // 2, 2, NX, 2 * ROWS * STEP), BF16),
            pltpu.VMEM((NY // 128, 256, NY), BF16),
            pltpu.VMEM((2, NZ, NZ), BF16),
            pltpu.VMEM((2, ROWS, 64, 128), F32),
            pltpu.VMEM((CHUNKS, ROWS, 2, YL, 128), F32),
            pltpu.VMEM((CHUNKS, ROWS, 2, YL, 128), F32),
            pltpu.VMEM((CHUNKS, COLS, 2, KY, 128), F32),
            pltpu.VMEM((CHUNKS, COLS, 2, KY, 128), F32),
            pltpu.VMEM((KY, NZ), F32),
            pltpu.SemaphoreType.DMA((10,)),
            pltpu.SemaphoreType.DMA,
            pltpu.SemaphoreType.DMA((CHUNKS, 2)),
            pltpu.SemaphoreType.DMA,
            pltpu.SemaphoreType.DMA((CHUNKS, 2)),
        ],
        compiler_params=pltpu.CompilerParams(collective_id=1, has_side_effects=True, vmem_limit_bytes=40 << 20),
        name="sine_modes",
    )(*(pltpu.with_memory_space_constraint(operand, pltpu.HBM) for operand in operands))


def solution(mesh):
    return jax.shard_map(
        local,
        mesh=mesh,
        in_specs=(P(None, None, "row", "col"), P(), P(), P(), P()),
        out_specs=P(None, "row", "col", None),
        check_vma=False,
    )
```

```python
import functools

import jax
import jax.numpy as jnp
import ml_dtypes
import numpy as np
from jax import lax
from jax.experimental import pallas as pl
from jax.experimental.pallas import tpu as pltpu
from jax.sharding import PartitionSpec as P

F32, BF16 = jnp.float32, jnp.bfloat16
MESH = pl.DeviceIdType.MESH
NX, NY, NZ, NF = 512, 512, 256, 2
RY, RX, CZ, CC = 4, 4, 4, 2
ROWS, COLS = RY * RX, CZ * CC
KX, KY = NX // ROWS, NY // COLS
YL, ZL = NY // ROWS, NZ // COLS
STEP = 8
PARTS = KX // STEP
CHUNKS = PARTS * NF
AHEAD, LAG_Z = 3, 3
ROW_ORDER = (10, 6, 9, 11, 14, 5, 15, 7, 13, 2, 8, 1, 4, 3, 12)
COL_ORDER = (4, 5, 2, 6, 3, 7, 1)


def mode_table(count):
    rank = np.arange(1, count + 1)
    turns = np.outer(rank, rank) % (2 * count + 2)
    return np.sin(np.pi / (count + 1) * turns) * np.sqrt(2.0 / (count + 1))


def two_terms(table):
    high = table.astype(np.float32).astype(ml_dtypes.bfloat16)
    low = (table - high.astype(np.float64)).astype(np.float32).astype(ml_dtypes.bfloat16)
    return high, low


def tables():
    high, low = two_terms(mode_table(NX))
    pick = lambda t: t.reshape(NX, ROWS, PARTS // 2, 2, STEP).transpose(2, 0, 3, 1, 4).reshape(PARTS // 2, NX, 2 * ROWS * STEP)
    table_x = np.stack([pick(high), pick(low)], axis=1)
    high, low = two_terms(mode_table(NY))
    swap = lambda t: t.reshape(NY // 128, 128, ROWS, YL // 4, 4).transpose(0, 1, 2, 4, 3).reshape(NY // 128, 128, NY)
    table_y = np.concatenate([swap(high), swap(low)], axis=1)
    table_z = np.stack(two_terms(mode_table(NZ)))
    return table_x, table_y, table_z


def split(values):
    high = values.astype(BF16)
    return high, (values - high.astype(F32)).astype(BF16)


def dot(a, b, b_dim=0):
    return lax.dot_general(a, b, (((1,), (b_dim,)), ((), ())), preferred_element_type=F32)


def exchange_groups(values):
    lane = lax.broadcasted_iota(jnp.int32, values[0].shape, 1)
    low_half, even = lane < 64, lane % 64 < 32
    a, b, c, d = values
    a, c = jnp.where(low_half, a, pltpu.roll(c, 64, 1)), jnp.where(low_half, pltpu.roll(a, 64, 1), c)
    b, d = jnp.where(low_half, b, pltpu.roll(d, 64, 1)), jnp.where(low_half, pltpu.roll(b, 64, 1), d)
    a, b = jnp.where(even, a, pltpu.roll(b, 32, 1)), jnp.where(even, pltpu.roll(a, 96, 1), b)
    c, d = jnp.where(even, c, pltpu.roll(d, 32, 1)), jnp.where(even, pltpu.roll(c, 96, 1), d)
    return a, b, c, d


def kernel(
    coupling_far, sym_x_far, sym_y_far, sym_z_far, field, table_x, table_y, table_z, result,
    coupling, sym_x, sym_y, sym_z, raw, tx, ty, tz, turn, row_out, row_in, col_out, col_in, base,
    load_sem, row_send, row_recv, col_send, col_recv,
):
    row, col = lax.axis_index("row"), lax.axis_index("col")
    row_peers = [(row // RX + s // RX) % RY * RX + (row + s % RX) % RX for s in ROW_ORDER]
    col_peers = [(col // CC + s // CC) % CZ * CC + (col + s % CC) % CC for s in COL_ORDER]
    last = CHUNKS - 1

    pieces = [pl.ds(n * 128, 128) for n in range(YL // 4)]
    pairs = [(table_x.at[0], tx.at[0])] + [(field.at[0, piece], raw.at[0, piece]) for piece in pieces]
    pairs += [(field.at[1], raw.at[1]), (table_x.at[1], tx.at[1])]
    pairs += [(table_y, ty), (table_z, tz), (sym_y_far, sym_y), (sym_z_far, sym_z), (sym_x_far, sym_x), (coupling_far, coupling)]
    loads = [pltpu.make_async_copy(src, dst, load_sem.at[n]) for n, (src, dst) in enumerate(pairs)]
    for load in loads:
        load.start()

    barrier = pltpu.get_barrier_semaphore()
    for peer in row_peers:
        pl.semaphore_signal(barrier, inc=1, device_id=(peer, col), device_id_type=MESH)
    for peer in col_peers:
        pl.semaphore_signal(barrier, inc=1, device_id=(row, peer), device_id_type=MESH)

    def wait_bytes(ref, sem):
        pltpu.make_async_copy(ref, ref, sem).wait()

    def make_base():
        for block in range(NY // 128):
            lanes = jnp.transpose(jnp.broadcast_to(sym_y[:, block * 128:(block + 1) * 128], (128, 128)))

            @pl.when(col // 2 == block)
            def _():
                mine = jnp.where(col % 2 == 0, lanes[0:64], lanes[64:128])
                base[...] = 1.0 + jnp.concatenate([mine, mine], axis=1) + sym_z[...]

    def row_exchange(i, kbs, sem):
        for peer in row_peers:
            pltpu.make_async_remote_copy(
                src_ref=row_out.at[i, peer, *kbs], dst_ref=row_in.at[i, row, *kbs], send_sem=row_send, recv_sem=sem,
                device_id=(peer, col), device_id_type=MESH,
            ).start()
        pltpu.make_async_copy(row_out.at[i, row, *kbs], row_in.at[i, row, *kbs], sem).start()

    def col_exchange(i, kbs, sem):
        for peer in col_peers:
            pltpu.make_async_remote_copy(
                src_ref=col_out.at[i, peer, *kbs], dst_ref=col_in.at[i, col, *kbs], send_sem=col_send, recv_sem=sem,
                device_id=(row, peer), device_id_type=MESH,
            ).start()
        pltpu.make_async_copy(col_out.at[i, col, *kbs], col_in.at[i, col, *kbs], sem).start()

    def x_step(u):
        h, a = u // 2, u % 2
        for n, when in ((0, 0), *((1 + k, 0) for k in range(8)), (9, 1), (10, 2)):
            pl.when(u == when)(loads[n].wait)

        def lines(n, carry):
            rows = pl.ds(pl.multiple_of(n * 128, 128), 128)
            high, low = split(raw[a, rows, :])
            both = dot(jnp.concatenate([high, low], axis=0), tx[h, 0])
            values = both[:128] + both[128:] + dot(high, tx[h, 1])
            for b in range(2):
                flipped = jnp.transpose(values[:, b * 128:(b + 1) * 128])
                for r in range(ROWS):
                    turn[b, r, pl.ds(n, 8, stride=8), :] = flipped[r * 8:(r + 1) * 8]
            return carry
        lax.fori_loop(0, YL // 4, lines, 0, unroll=8)

        for b in range(2):
            i = 2 * u + b
            for kb in range(2):
                for r in range(0, ROWS, 4):
                    parts = [turn[b, r:r + 4, (kb * 4 + k) * 8:(kb * 4 + k + 1) * 8, :].reshape(32, 128) for k in range(4)]
                    for g, part in enumerate(exchange_groups(parts)):
                        row_out[i, r:r + 4, kb, g * 8:(g + 1) * 8, :] = part.reshape(4, 8, 128)
                if b * 2 + kb < AHEAD:
                    @pl.when(u == 0)
                    def _():
                        if b == 0 and kb == 0:
                            pl.semaphore_wait(barrier, ROWS + COLS - 2)
                        row_exchange(i, (kb,), row_recv.at[i, kb])

    def y_step(i, kb, count):
        kbs = pl.ds(kb, count)
        wait_bytes(row_in.at[i, :, kbs], row_recv.at[i, kb])
        lines = jnp.concatenate([row_in[i, :, kb + k].reshape(NY, 128) for k in range(count)], axis=1)
        high, low = split(lines)
        for m in range(NY // 128):
            both = dot(ty[m], high)
            values = both[:128] + both[128:] + dot(ty[m, 0:128], low)
            for k in range(count):
                col_out[i, 2 * m:2 * m + 2, kb + k] = values[:, k * 128:(k + 1) * 128].reshape(2, KY, 128)
        col_exchange(i, (kb,) if count == 1 else (), col_recv.at[i, kb])

    def z_wait(i, kb, count):
        wait_bytes(col_in.at[i, :, pl.ds(kb, count)], col_recv.at[i, kb])

    def z_step(i, kb, count):
        a, first_x = i // 2 % 2, (i // 4 * 2 + i % 2) * STEP + kb * 4
        for k in range(count):
            halves = [exchange_groups([col_in[i, g * 4 + j, kb + k] for j in range(4)]) for g in range(2)]
            for pair in range(2):
                lines = [jnp.concatenate([halves[0][2 * pair + e], halves[1][2 * pair + e]], axis=1) for e in range(2)]
                high, low = split(jnp.concatenate(lines, axis=0))
                both = dot(jnp.concatenate([high, low], axis=0), tz[0])
                values = both[:128] + both[128:] + dot(high, tz[1])
                x = first_x + k * 4 + 2 * pair
                result[a, pl.ds(x, 2)] = values.reshape(2, KY, NZ)

        @pl.when(a == 1)
        def _():
            def mix(n, carry):
                x = first_x + n
                one, two = result[0, x], result[1, x]
                weight = 1.0 / (base[...] + sym_x[row * KX + x])
                rest = 1.0 - weight
                result[0, x] = weight * one + rest * (coupling[0, 0] * one + coupling[0, 1] * two)
                result[1, x] = weight * two + rest * (coupling[1, 0] * one + coupling[1, 1] * two)
                return carry
            lax.fori_loop(0, 4 * count, mix, 0)

    def halves(step):
        def body(kb, carry):
            step(kb)
            return carry
        lax.fori_loop(0, 2, body, 0)

    lag = LAG_Z

    def send(j):
        @pl.when(j < 2 * CHUNKS)
        def _():
            row_exchange(j // 2, (j % 2,), row_recv.at[j // 2, j % 2])

    def middle(j, carry):
        pl.when(jnp.logical_or(j == 2, j == 6))(lambda: x_step((j + 6) // 4))
        send(j + AHEAD)
        y_step(j // 2, j % 2, 1)

        @pl.when(j >= lag)
        def _():
            z_wait((j - lag) // 2, (j - lag) % 2, 1)
            z_step((j - lag) // 2, (j - lag) % 2, 1)
        return carry

    halves(x_step)
    for load in loads[11:]:
        load.wait()
    make_base()
    lax.fori_loop(0, 2 * CHUNKS, middle, 0)

    def final(j, carry):
        z_wait(j // 2, j % 2, 1)
        z_step(j // 2, j % 2, 1)
        return carry
    lax.fori_loop(2 * CHUNKS - lag, 2 * CHUNKS, final, 0)
    wait_bytes(row_out.at[:, pl.ds(0, ROWS - 1)], row_send)
    wait_bytes(col_out.at[:, pl.ds(0, COLS - 1)], col_send)


def local(species, coupling, symbol_x, symbol_y, symbol_z):
    field = jnp.transpose(species, (0, 2, 3, 1)).reshape(NF, YL * ZL, NX)
    operands = (coupling, symbol_x, symbol_y.reshape(1, NY), symbol_z.reshape(1, NZ), field, *map(jnp.asarray, tables()))
    far = pl.BlockSpec(memory_space=pltpu.HBM)
    return pl.pallas_call(
        kernel,
        out_shape=pltpu.VMEM((NF, KX, KY, NZ), F32),
        in_specs=[far] * 8,
        out_specs=pl.BlockSpec(memory_space=pltpu.VMEM),
        scratch_shapes=[
            pltpu.SMEM((NF, NF), F32),
            pltpu.SMEM((NX,), F32),
            pltpu.VMEM((1, NY), F32),
            pltpu.VMEM((1, NZ), F32),
            pltpu.VMEM((NF, YL * ZL, NX), F32),
            pltpu.VMEM((PARTS // 2, 2, NX, 2 * ROWS * STEP), BF16),
            pltpu.VMEM((NY // 128, 256, NY), BF16),
            pltpu.VMEM((2, NZ, NZ), BF16),
            pltpu.VMEM((2, ROWS, 64, 128), F32),
            pltpu.VMEM((CHUNKS, ROWS, 2, YL, 128), F32),
            pltpu.VMEM((CHUNKS, ROWS, 2, YL, 128), F32),
            pltpu.VMEM((CHUNKS, COLS, 2, KY, 128), F32),
            pltpu.VMEM((CHUNKS, COLS, 2, KY, 128), F32),
            pltpu.VMEM((KY, NZ), F32),
            pltpu.SemaphoreType.DMA((17,)),
            pltpu.SemaphoreType.DMA,
            pltpu.SemaphoreType.DMA((CHUNKS, 2)),
            pltpu.SemaphoreType.DMA,
            pltpu.SemaphoreType.DMA((CHUNKS, 2)),
        ],
        compiler_params=pltpu.CompilerParams(collective_id=1, has_side_effects=True, vmem_limit_bytes=40 << 20),
        name="sine_modes",
    )(*(pltpu.with_memory_space_constraint(operand, pltpu.HBM) for operand in operands))


def solution(mesh):
    return jax.shard_map(
        local,
        mesh=mesh,
        in_specs=(P(None, None, "row", "col"), P(), P(), P(), P()),
        out_specs=P(None, "row", "col", None),
        check_vma=False,
    )
```

```python
import functools

import jax
import jax.numpy as jnp
import ml_dtypes
import numpy as np
from jax import lax
from jax.experimental import pallas as pl
from jax.experimental.pallas import tpu as pltpu
from jax.sharding import PartitionSpec as P

F32, BF16 = jnp.float32, jnp.bfloat16
MESH = pl.DeviceIdType.MESH
NX, NY, NZ, NF = 512, 512, 256, 2
RY, RX, CZ, CC = 4, 4, 4, 2
ROWS, COLS = RY * RX, CZ * CC
KX, KY = NX // ROWS, NY // COLS
YL, ZL = NY // ROWS, NZ // COLS
STEP = 8
PARTS = KX // STEP
CHUNKS = PARTS * NF
AHEAD, LAG_Z = 3, 3
ROW_ORDER = (10, 6, 9, 11, 14, 5, 15, 7, 13, 2, 8, 1, 4, 3, 12)
COL_ORDER = (5, 4, 3, 7, 2, 6, 1)


def mode_table(count):
    rank = np.arange(1, count + 1)
    turns = np.outer(rank, rank) % (2 * count + 2)
    return np.sin(np.pi / (count + 1) * turns) * np.sqrt(2.0 / (count + 1))


def two_terms(table):
    high = table.astype(np.float32).astype(ml_dtypes.bfloat16)
    low = (table - high.astype(np.float64)).astype(np.float32).astype(ml_dtypes.bfloat16)
    return high, low


def tables():
    high, low = two_terms(mode_table(NX))
    pick = lambda t: t.reshape(NX, ROWS, PARTS // 2, 2, STEP).transpose(2, 0, 3, 1, 4).reshape(PARTS // 2, NX, 2 * ROWS * STEP)
    table_x = np.stack([pick(high), pick(low)], axis=1)
    high, low = two_terms(mode_table(NY))
    swap = lambda t: t.reshape(NY // 128, 128, ROWS, YL // 4, 4).transpose(0, 1, 2, 4, 3).reshape(NY // 128, 128, NY)
    table_y = np.concatenate([swap(high), swap(low)], axis=1)
    table_z = np.stack(two_terms(mode_table(NZ)))
    return table_x, table_y, table_z


def split(values):
    high = values.astype(BF16)
    return high, (values - high.astype(F32)).astype(BF16)


def dot(a, b, b_dim=0):
    return lax.dot_general(a, b, (((1,), (b_dim,)), ((), ())), preferred_element_type=F32)


def exchange_groups(values):
    lane = lax.broadcasted_iota(jnp.int32, values[0].shape, 1)
    low_half, even = lane < 64, lane % 64 < 32
    a, b, c, d = values
    a, c = jnp.where(low_half, a, pltpu.roll(c, 64, 1)), jnp.where(low_half, pltpu.roll(a, 64, 1), c)
    b, d = jnp.where(low_half, b, pltpu.roll(d, 64, 1)), jnp.where(low_half, pltpu.roll(b, 64, 1), d)
    a, b = jnp.where(even, a, pltpu.roll(b, 32, 1)), jnp.where(even, pltpu.roll(a, 96, 1), b)
    c, d = jnp.where(even, c, pltpu.roll(d, 32, 1)), jnp.where(even, pltpu.roll(c, 96, 1), d)
    return a, b, c, d


def kernel(
    coupling_far, sym_x_far, sym_y_far, sym_z_far, field, table_x, table_y, table_z, result,
    coupling, sym_x, sym_y, sym_z, raw, tx, ty, tz, turn, row_out, row_in, col_out, col_in, base,
    load_sem, row_send, row_recv, col_send, col_recv,
):
    row, col = lax.axis_index("row"), lax.axis_index("col")
    turn_of = 1 + 2 * (col % 2)
    row_peers = [(row // RX + s // RX * turn_of) % RY * RX + (row + s % RX * turn_of) % RX for s in ROW_ORDER]
    turn_of = 1 + 2 * (col % 2)
    col_peers = [(col // CC + s // CC * turn_of) % CZ * CC + (col + s % CC) % CC for s in COL_ORDER]
    last = CHUNKS - 1

    pieces = [pl.ds(n * 512, 512) for n in range(2)]
    pairs = [(table_x.at[0], tx.at[0])] + [(field.at[0, piece], raw.at[0, piece]) for piece in pieces]
    pairs += [(field.at[1], raw.at[1]), (table_x.at[1], tx.at[1])]
    pairs += [(table_y, ty), (table_z, tz), (sym_y_far, sym_y), (sym_z_far, sym_z), (sym_x_far, sym_x), (coupling_far, coupling)]
    loads = [pltpu.make_async_copy(src, dst, load_sem.at[n]) for n, (src, dst) in enumerate(pairs)]
    for load in loads[:3]:
        load.start()

    barrier = pltpu.get_barrier_semaphore()
    for peer in row_peers:
        pl.semaphore_signal(barrier, inc=1, device_id=(peer, col), device_id_type=MESH)
    for peer in col_peers:
        pl.semaphore_signal(barrier, inc=1, device_id=(row, peer), device_id_type=MESH)

    def wait_bytes(ref, sem):
        pltpu.make_async_copy(ref, ref, sem).wait()

    def make_base():
        for block in range(NY // 128):
            lanes = jnp.transpose(jnp.broadcast_to(sym_y[:, block * 128:(block + 1) * 128], (128, 128)))

            @pl.when(col // 2 == block)
            def _():
                mine = jnp.where(col % 2 == 0, lanes[0:64], lanes[64:128])
                base[...] = 1.0 + jnp.concatenate([mine, mine], axis=1) + sym_z[...]

    def row_exchange(i, kbs, sem):
        for peer in row_peers:
            pltpu.make_async_remote_copy(
                src_ref=row_out.at[i, peer, *kbs], dst_ref=row_in.at[i, row, *kbs], send_sem=row_send, recv_sem=sem,
                device_id=(peer, col), device_id_type=MESH,
            ).start()
        pltpu.make_async_copy(row_out.at[i, row, *kbs], row_in.at[i, row, *kbs], sem).start()

    def col_exchange(i, kbs, sem):
        for peer in col_peers:
            pltpu.make_async_remote_copy(
                src_ref=col_out.at[i, peer, *kbs], dst_ref=col_in.at[i, col, *kbs], send_sem=col_send, recv_sem=sem,
                device_id=(row, peer), device_id_type=MESH,
            ).start()
        pltpu.make_async_copy(col_out.at[i, col, *kbs], col_in.at[i, col, *kbs], sem).start()

    def x_step(u):
        h, a = u // 2, u % 2
        for n, when in ((0, 0), (1, 0), (2, 0), (3, 1), (4, 2)):
            pl.when(u == when)(loads[n].wait)

        @pl.when(u == 0)
        def _():
            for load in loads[3:]:
                load.start()

        def lines(n, carry):
            rows = pl.ds(pl.multiple_of(n * 128, 128), 128)
            high, low = split(raw[a, rows, :])
            both = dot(jnp.concatenate([high, low], axis=0), tx[h, 0])
            values = both[:128] + both[128:] + dot(high, tx[h, 1])
            for b in range(2):
                flipped = jnp.transpose(values[:, b * 128:(b + 1) * 128])
                for r in range(ROWS):
                    turn[b, r, pl.ds(n, 8, stride=8), :] = flipped[r * 8:(r + 1) * 8]
            return carry
        lax.fori_loop(0, YL // 4, lines, 0, unroll=8)

        for b in range(2):
            i = 2 * u + b
            for kb in range(2):
                for r in range(0, ROWS, 4):
                    parts = [turn[b, r:r + 4, (kb * 4 + k) * 8:(kb * 4 + k + 1) * 8, :].reshape(32, 128) for k in range(4)]
                    for g, part in enumerate(exchange_groups(parts)):
                        row_out[i, r:r + 4, kb, g * 8:(g + 1) * 8, :] = part.reshape(4, 8, 128)
                if b * 2 + kb < AHEAD:
                    @pl.when(u == 0)
                    def _():
                        if b == 0 and kb == 0:
                            pl.semaphore_wait(barrier, ROWS + COLS - 2)
                        row_exchange(i, (kb,), row_recv.at[i, kb])

    def y_step(i, kb, count):
        kbs = pl.ds(kb, count)
        wait_bytes(row_in.at[i, :, kbs], row_recv.at[i, kb])
        lines = jnp.concatenate([row_in[i, :, kb + k].reshape(NY, 128) for k in range(count)], axis=1)
        high, low = split(lines)
        terms = jnp.concatenate([high, low], axis=1)
        for m in range(NY // 128):
            four = dot(ty[m], terms)
            values = four[:128, :128] + (four[128:, :128] + four[:128, 128:])
            col_out[i, 2 * m:2 * m + 2, kb] = values.reshape(2, KY, 128)
        col_exchange(i, (kb,), col_recv.at[i, kb])

    def z_wait(i, kb, count):
        wait_bytes(col_in.at[i, :, pl.ds(kb, count)], col_recv.at[i, kb])

    def z_step(i, kb, count):
        a, first_x = i // 2 % 2, (i // 4 * 2 + i % 2) * STEP + kb * 4
        for k in range(count):
            halves = [exchange_groups([col_in[i, g * 4 + j, kb + k] for j in range(4)]) for g in range(2)]
            for pair in range(2):
                lines = [jnp.concatenate([halves[0][2 * pair + e], halves[1][2 * pair + e]], axis=1) for e in range(2)]
                high, low = split(jnp.concatenate(lines, axis=0))
                both = dot(jnp.concatenate([high, low], axis=0), tz[0])
                values = both[:128] + both[128:] + dot(high, tz[1])
                x = first_x + k * 4 + 2 * pair
                result[a, pl.ds(x, 2)] = values.reshape(2, KY, NZ)

        @pl.when(a == 1)
        def _():
            def mix(n, carry):
                x = first_x + n
                one, two = result[0, x], result[1, x]
                weight = 1.0 / (base[...] + sym_x[row * KX + x])
                rest = 1.0 - weight
                result[0, x] = weight * one + rest * (coupling[0, 0] * one + coupling[0, 1] * two)
                result[1, x] = weight * two + rest * (coupling[1, 0] * one + coupling[1, 1] * two)
                return carry
            lax.fori_loop(0, 4 * count, mix, 0, unroll=4)

    def halves(step):
        def body(kb, carry):
            step(kb)
            return carry
        lax.fori_loop(0, 2, body, 0)

    lag = LAG_Z

    def send(j):
        @pl.when(j < 2 * CHUNKS)
        def _():
            row_exchange(j // 2, (j % 2,), row_recv.at[j // 2, j % 2])

    def middle(j, carry):
        pl.when(jnp.logical_or(j == 2, j == 6))(lambda: x_step((j + 6) // 4))
        send(j + AHEAD)
        y_step(j // 2, j % 2, 1)

        @pl.when(j >= lag)
        def _():
            z_wait((j - lag) // 2, (j - lag) % 2, 1)
            z_step((j - lag) // 2, (j - lag) % 2, 1)
        return carry

    halves(x_step)
    for load in loads[5:]:
        load.wait()
    make_base()
    lax.fori_loop(0, 2 * CHUNKS, middle, 0)

    def final(j, carry):
        z_wait(j // 2, j % 2, 1)
        z_step(j // 2, j % 2, 1)
        return carry
    lax.fori_loop(2 * CHUNKS - lag, 2 * CHUNKS, final, 0)
    wait_bytes(row_out.at[:, pl.ds(0, ROWS - 1)], row_send)
    wait_bytes(col_out.at[:, pl.ds(0, COLS - 1)], col_send)


def local(species, coupling, symbol_x, symbol_y, symbol_z):
    field = jnp.transpose(species, (0, 2, 3, 1)).reshape(NF, YL * ZL, NX)
    operands = (coupling, symbol_x, symbol_y.reshape(1, NY), symbol_z.reshape(1, NZ), field, *map(jnp.asarray, tables()))
    far = pl.BlockSpec(memory_space=pltpu.HBM)
    return pl.pallas_call(
        kernel,
        out_shape=pltpu.VMEM((NF, KX, KY, NZ), F32),
        in_specs=[far] * 8,
        out_specs=pl.BlockSpec(memory_space=pltpu.VMEM),
        scratch_shapes=[
            pltpu.SMEM((NF, NF), F32),
            pltpu.SMEM((NX,), F32),
            pltpu.VMEM((1, NY), F32),
            pltpu.VMEM((1, NZ), F32),
            pltpu.VMEM((NF, YL * ZL, NX), F32),
            pltpu.VMEM((PARTS // 2, 2, NX, 2 * ROWS * STEP), BF16),
            pltpu.VMEM((NY // 128, 256, NY), BF16),
            pltpu.VMEM((2, NZ, NZ), BF16),
            pltpu.VMEM((2, ROWS, 64, 128), F32),
            pltpu.VMEM((CHUNKS, ROWS, 2, YL, 128), F32),
            pltpu.VMEM((CHUNKS, ROWS, 2, YL, 128), F32),
            pltpu.VMEM((CHUNKS, COLS, 2, KY, 128), F32),
            pltpu.VMEM((CHUNKS, COLS, 2, KY, 128), F32),
            pltpu.VMEM((KY, NZ), F32),
            pltpu.SemaphoreType.DMA((11,)),
            pltpu.SemaphoreType.DMA,
            pltpu.SemaphoreType.DMA((CHUNKS, 2)),
            pltpu.SemaphoreType.DMA,
            pltpu.SemaphoreType.DMA((CHUNKS, 2)),
        ],
        compiler_params=pltpu.CompilerParams(collective_id=1, has_side_effects=True, vmem_limit_bytes=40 << 20),
        name="sine_modes",
    )(*(pltpu.with_memory_space_constraint(operand, pltpu.HBM) for operand in operands))


def solution(mesh):
    return jax.shard_map(
        local,
        mesh=mesh,
        in_specs=(P(None, None, "row", "col"), P(), P(), P(), P()),
        out_specs=P(None, "row", "col", None),
        check_vma=False,
    )
```

```python
import functools

import jax
import jax.numpy as jnp
import ml_dtypes
import numpy as np
from jax import lax
from jax.experimental import pallas as pl
from jax.experimental.pallas import tpu as pltpu
from jax.sharding import PartitionSpec as P

F32, BF16 = jnp.float32, jnp.bfloat16
MESH = pl.DeviceIdType.MESH
NX, NY, NZ, NF = 512, 512, 256, 2
RY, RX, CZ, CC = 4, 4, 4, 2
ROWS, COLS = RY * RX, CZ * CC
KX, KY = NX // ROWS, NY // COLS
YL, ZL = NY // ROWS, NZ // COLS
STEP = 8
PARTS = KX // STEP
CHUNKS = PARTS * NF
AHEAD, LAG_Z = 3, 3
ROW_ORDER = (10, 6, 9, 11, 14, 5, 15, 7, 13, 2, 8, 1, 4, 3, 12)
COL_ORDER = (5, 3, 7, 4, 2, 6, 1)


def mode_table(count):
    rank = np.arange(1, count + 1)
    turns = np.outer(rank, rank) % (2 * count + 2)
    return np.sin(np.pi / (count + 1) * turns) * np.sqrt(2.0 / (count + 1))


def two_terms(table):
    high = table.astype(np.float32).astype(ml_dtypes.bfloat16)
    low = (table - high.astype(np.float64)).astype(np.float32).astype(ml_dtypes.bfloat16)
    return high, low


def tables():
    high, low = two_terms(mode_table(NX))
    pick = lambda t: t.reshape(NX, ROWS, PARTS // 2, 2, STEP).transpose(2, 0, 3, 1, 4).reshape(PARTS // 2, NX, 2 * ROWS * STEP)
    table_x = np.stack([pick(high), pick(low)], axis=1)
    high, low = two_terms(mode_table(NY))
    swap = lambda t: t.reshape(NY // 128, 128, ROWS, YL // 4, 4).transpose(0, 1, 2, 4, 3).reshape(NY // 128, 128, NY)
    table_y = np.concatenate([swap(high), swap(low)], axis=1)
    table_z = np.stack(two_terms(mode_table(NZ)))
    return table_x, table_y, table_z


def split(values):
    high = values.astype(BF16)
    return high, (values - high.astype(F32)).astype(BF16)


def dot(a, b, b_dim=0):
    return lax.dot_general(a, b, (((1,), (b_dim,)), ((), ())), preferred_element_type=F32)


def exchange_groups(values):
    lane = lax.broadcasted_iota(jnp.int32, values[0].shape, 1)
    low_half, even = lane < 64, lane % 64 < 32
    a, b, c, d = values
    a, c = jnp.where(low_half, a, pltpu.roll(c, 64, 1)), jnp.where(low_half, pltpu.roll(a, 64, 1), c)
    b, d = jnp.where(low_half, b, pltpu.roll(d, 64, 1)), jnp.where(low_half, pltpu.roll(b, 64, 1), d)
    a, b = jnp.where(even, a, pltpu.roll(b, 32, 1)), jnp.where(even, pltpu.roll(a, 96, 1), b)
    c, d = jnp.where(even, c, pltpu.roll(d, 32, 1)), jnp.where(even, pltpu.roll(c, 96, 1), d)
    return a, b, c, d


def z_transform(piece, table):
    groups = [exchange_groups([piece(g * 4 + j) for j in range(4)]) for g in range(2)]
    for pair in range(2):
        lines = [jnp.concatenate([groups[0][2 * pair + e], groups[1][2 * pair + e]], axis=1) for e in range(2)]
        high, low = split(jnp.concatenate(lines, axis=0))
        both = dot(jnp.concatenate([high, low], axis=0), table[0])
        yield both[:128] + both[128:] + dot(high, table[1])


def finish(result, tail, table, weights, mixing, out, mixed, sem):
    done = KX - 4
    copies = [pltpu.make_async_copy(result.at[a, pl.ds(0, done)], out.at[a, pl.ds(0, done)], sem.at[a]) for a in range(NF)]
    copies += [pltpu.make_async_copy(mixed.at[a], out.at[a, pl.ds(done, 4)], sem.at[NF + a]) for a in range(NF)]
    for copy in copies[:NF]:
        copy.start()
    for pair, values in enumerate(z_transform(lambda c: tail[c], table)):
        for e in range(2):
            x = 2 * pair + e
            one, two, weight = result[0, done + x], values[e * KY:(e + 1) * KY], weights[x]
            rest = 1.0 - weight
            mixed[0, x] = weight * one + rest * (mixing[0] * one + mixing[1] * two)
            mixed[1, x] = weight * two + rest * (mixing[2] * one + mixing[3] * two)
    for copy in copies[NF:]:
        copy.start()
    for copy in copies:
        copy.wait()


def kernel(
    coupling_far, sym_x_far, sym_y_far, sym_z_far, field, table_x, table_y, table_z, result, tail, tz, weights, mixing,
    coupling, sym_x, sym_y, sym_z, raw, tx, ty, turn, row_out, row_in, col_out, col_in, base,
    load_sem, row_send, row_recv, col_send, col_recv,
):
    row, col = lax.axis_index("row"), lax.axis_index("col")
    turn_of = 1 + 2 * (col % 2)
    row_peers = [(row // RX + s // RX * turn_of) % RY * RX + (row + s % RX * turn_of) % RX for s in ROW_ORDER]
    turn_of = 1 + 2 * (col % 2)
    col_peers = [(col // CC + s // CC * turn_of) % CZ * CC + (col + s % CC) % CC for s in COL_ORDER]
    last = CHUNKS - 1

    pieces = [pl.ds(n * 512, 512) for n in range(2)]
    pairs = [(table_x.at[0], tx.at[0])] + [(field.at[0, piece], raw.at[0, piece]) for piece in pieces]
    pairs += [(field.at[1], raw.at[1]), (table_x.at[1], tx.at[1])]
    pairs += [(table_y, ty), (table_z, tz), (sym_y_far, sym_y), (sym_z_far, sym_z), (sym_x_far, sym_x), (coupling_far, coupling)]
    loads = [pltpu.make_async_copy(src, dst, load_sem.at[n]) for n, (src, dst) in enumerate(pairs)]
    for load in loads[:3]:
        load.start()

    barrier = pltpu.get_barrier_semaphore()
    for peer in row_peers:
        pl.semaphore_signal(barrier, inc=1, device_id=(peer, col), device_id_type=MESH)
    for peer in col_peers:
        pl.semaphore_signal(barrier, inc=1, device_id=(row, peer), device_id_type=MESH)

    def wait_bytes(ref, sem):
        pltpu.make_async_copy(ref, ref, sem).wait()

    def make_base():
        for block in range(NY // 128):
            lanes = jnp.transpose(jnp.broadcast_to(sym_y[:, block * 128:(block + 1) * 128], (128, 128)))

            @pl.when(col // 2 == block)
            def _():
                mine = jnp.where(col % 2 == 0, lanes[0:64], lanes[64:128])
                base[...] = 1.0 + jnp.concatenate([mine, mine], axis=1) + sym_z[...]

    def row_exchange(i, kbs, sem):
        for peer in row_peers:
            pltpu.make_async_remote_copy(
                src_ref=row_out.at[i, peer, *kbs], dst_ref=row_in.at[i, row, *kbs], send_sem=row_send, recv_sem=sem,
                device_id=(peer, col), device_id_type=MESH,
            ).start()
        pltpu.make_async_copy(row_out.at[i, row, *kbs], row_in.at[i, row, *kbs], sem).start()

    def col_exchange(i, kbs, sem):
        for peer in col_peers:
            pltpu.make_async_remote_copy(
                src_ref=col_out.at[i, peer, *kbs], dst_ref=col_in.at[i, col, *kbs], send_sem=col_send, recv_sem=sem,
                device_id=(row, peer), device_id_type=MESH,
            ).start()
        pltpu.make_async_copy(col_out.at[i, col, *kbs], col_in.at[i, col, *kbs], sem).start()

    def x_step(u):
        h, a = u // 2, u % 2
        for n, when in ((0, 0), (1, 0), (2, 0), (3, 1), (4, 2)):
            pl.when(u == when)(loads[n].wait)

        @pl.when(u == 0)
        def _():
            for load in loads[3:]:
                load.start()

        def lines(n, carry):
            rows = pl.ds(pl.multiple_of(n * 128, 128), 128)
            high, low = split(raw[a, rows, :])
            both = dot(jnp.concatenate([high, low], axis=0), tx[h, 0])
            values = both[:128] + both[128:] + dot(high, tx[h, 1])
            for b in range(2):
                flipped = jnp.transpose(values[:, b * 128:(b + 1) * 128])
                for r in range(ROWS):
                    turn[b, r, pl.ds(n, 8, stride=8), :] = flipped[r * 8:(r + 1) * 8]
            return carry
        lax.fori_loop(0, YL // 4, lines, 0, unroll=8)

        for b in range(2):
            i = 2 * u + b
            for kb in range(2):
                for r in range(0, ROWS, 4):
                    parts = [turn[b, r:r + 4, (kb * 4 + k) * 8:(kb * 4 + k + 1) * 8, :].reshape(32, 128) for k in range(4)]
                    for g, part in enumerate(exchange_groups(parts)):
                        row_out[i, r:r + 4, kb, g * 8:(g + 1) * 8, :] = part.reshape(4, 8, 128)
                if b * 2 + kb < AHEAD:
                    @pl.when(u == 0)
                    def _():
                        if b == 0 and kb == 0:
                            pl.semaphore_wait(barrier, ROWS + COLS - 2)
                        row_exchange(i, (kb,), row_recv.at[i, kb])

    def y_step(i, kb, count):
        kbs = pl.ds(kb, count)
        wait_bytes(row_in.at[i, :, kbs], row_recv.at[i, kb])
        lines = jnp.concatenate([row_in[i, :, kb + k].reshape(NY, 128) for k in range(count)], axis=1)
        high, low = split(lines)
        terms = jnp.concatenate([high, low], axis=1)
        for m in range(NY // 128):
            four = dot(ty[m], terms)
            values = four[:128, :128] + (four[128:, :128] + four[:128, 128:])
            col_out[i, 2 * m:2 * m + 2, kb] = values.reshape(2, KY, 128)
        col_exchange(i, (kb,), col_recv.at[i, kb])

    def z_wait(i, kb, count):
        wait_bytes(col_in.at[i, :, pl.ds(kb, count)], col_recv.at[i, kb])

    def z_step(i, kb, count):
        a, first_x = i // 2 % 2, (i // 4 * 2 + i % 2) * STEP + kb * 4
        for k in range(count):
            for pair, values in enumerate(z_transform(lambda c: col_in[i, c, kb + k], tz)):
                result[a, pl.ds(first_x + k * 4 + 2 * pair, 2)] = values.reshape(2, KY, NZ)

        @pl.when(a == 1)
        def _():
            def mix(n, carry):
                x = first_x + n
                one, two = result[0, x], result[1, x]
                weight = 1.0 / (base[...] + sym_x[row * KX + x])
                rest = 1.0 - weight
                result[0, x] = weight * one + rest * (coupling[0, 0] * one + coupling[0, 1] * two)
                result[1, x] = weight * two + rest * (coupling[1, 0] * one + coupling[1, 1] * two)
                return carry
            lax.fori_loop(0, 4 * count, mix, 0, unroll=4)

    def halves(step):
        def body(kb, carry):
            step(kb)
            return carry
        lax.fori_loop(0, 2, body, 0)

    lag = LAG_Z

    def send(j):
        @pl.when(j < 2 * CHUNKS)
        def _():
            row_exchange(j // 2, (j % 2,), row_recv.at[j // 2, j % 2])

    def middle(j, carry):
        pl.when(jnp.logical_or(j == 2, j == 6))(lambda: x_step((j + 6) // 4))
        send(j + AHEAD)
        y_step(j // 2, j % 2, 1)

        @pl.when(j >= lag)
        def _():
            z_wait((j - lag) // 2, (j - lag) % 2, 1)
            z_step((j - lag) // 2, (j - lag) % 2, 1)
        return carry

    halves(x_step)
    for load in loads[5:]:
        load.wait()
    make_base()
    for x in range(4):
        weights[x] = 1.0 / (base[...] + sym_x[row * KX + KX - 4 + x])
    for n in range(NF * NF):
        mixing[n] = jnp.full((KY, NZ), coupling[n // NF, n % NF], F32)
    lax.fori_loop(0, 2 * CHUNKS, middle, 0)

    def final(j, carry):
        z_wait(j // 2, j % 2, 1)
        z_step(j // 2, j % 2, 1)
        return carry
    lax.fori_loop(2 * CHUNKS - lag, 2 * CHUNKS - 1, final, 0)
    z_wait(last, 1, 1)
    tail[...] = col_in[last, :, 1]
    wait_bytes(row_out.at[:, pl.ds(0, ROWS - 1)], row_send)
    wait_bytes(col_out.at[:, pl.ds(0, COLS - 1)], col_send)


def local(species, coupling, symbol_x, symbol_y, symbol_z):
    field = jnp.transpose(species, (0, 2, 3, 1)).reshape(NF, YL * ZL, NX)
    operands = (coupling, symbol_x, symbol_y.reshape(1, NY), symbol_z.reshape(1, NZ), field, *map(jnp.asarray, tables()))
    far = pl.BlockSpec(memory_space=pltpu.HBM)
    parts = pl.pallas_call(
        kernel,
        out_shape=[
            pltpu.VMEM((NF, KX, KY, NZ), F32),
            pltpu.VMEM((COLS, KY, 128), F32),
            pltpu.VMEM((2, NZ, NZ), BF16),
            pltpu.VMEM((4, KY, NZ), F32),
            pltpu.VMEM((NF * NF, KY, NZ), F32),
        ],
        in_specs=[far] * 8,
        out_specs=[pl.BlockSpec(memory_space=pltpu.VMEM)] * 5,
        scratch_shapes=[
            pltpu.SMEM((NF, NF), F32),
            pltpu.SMEM((NX,), F32),
            pltpu.VMEM((1, NY), F32),
            pltpu.VMEM((1, NZ), F32),
            pltpu.VMEM((NF, YL * ZL, NX), F32),
            pltpu.VMEM((PARTS // 2, 2, NX, 2 * ROWS * STEP), BF16),
            pltpu.VMEM((NY // 128, 256, NY), BF16),
            pltpu.VMEM((2, ROWS, 72, 128), F32),
            pltpu.VMEM((CHUNKS, ROWS, 2, YL, 128), F32),
            pltpu.VMEM((CHUNKS, ROWS, 2, YL, 128), F32),
            pltpu.VMEM((CHUNKS, COLS, 2, KY, 128), F32),
            pltpu.VMEM((CHUNKS, COLS, 2, KY, 128), F32),
            pltpu.VMEM((KY, NZ), F32),
            pltpu.SemaphoreType.DMA((11,)),
            pltpu.SemaphoreType.DMA,
            pltpu.SemaphoreType.DMA((CHUNKS, 2)),
            pltpu.SemaphoreType.DMA,
            pltpu.SemaphoreType.DMA((CHUNKS, 2)),
        ],
        compiler_params=pltpu.CompilerParams(collective_id=1, has_side_effects=True, vmem_limit_bytes=40 << 20),
        name="sine_modes",
    )(*(pltpu.with_memory_space_constraint(operand, pltpu.HBM) for operand in operands))
    return pl.pallas_call(
        finish,
        out_shape=pltpu.HBM((NF, KX, KY, NZ), F32),
        in_specs=[pl.BlockSpec(memory_space=pltpu.VMEM)] * 5,
        out_specs=far,
        scratch_shapes=[pltpu.VMEM((NF, 4, KY, NZ), F32), pltpu.SemaphoreType.DMA((2 * NF,))],
        compiler_params=pltpu.CompilerParams(vmem_limit_bytes=8 << 20),
        name="finish",
    )(*(pltpu.with_memory_space_constraint(part, pltpu.VMEM) for part in parts))


def solution(mesh):
    return jax.shard_map(
        local,
        mesh=mesh,
        in_specs=(P(None, None, "row", "col"), P(), P(), P(), P()),
        out_specs=P(None, "row", "col", None),
        check_vma=False,
    )
```

```python
import functools

import jax
import jax.numpy as jnp
import ml_dtypes
import numpy as np
from jax import lax
from jax.experimental import pallas as pl
from jax.experimental.pallas import tpu as pltpu
from jax.sharding import PartitionSpec as P

F32, BF16 = jnp.float32, jnp.bfloat16
MESH = pl.DeviceIdType.MESH
NX, NY, NZ, NF = 512, 512, 256, 2
RY, RX, CZ, CC = 4, 4, 4, 2
ROWS, COLS = RY * RX, CZ * CC
KX, KY = NX // ROWS, NY // COLS
YL, ZL = NY // ROWS, NZ // COLS
STEP = 8
PARTS = KX // STEP
CHUNKS = PARTS * NF
AHEAD, LAG_Z = 3, 3
ROW_ORDER = (10, 6, 9, 14, 11, 2, 8, 5, 15, 7, 13, 1, 4, 3, 12)
COL_ORDER = (5, 3, 7, 4, 2, 6, 1)


def mode_table(count):
    rank = np.arange(1, count + 1)
    turns = np.outer(rank, rank) % (2 * count + 2)
    return np.sin(np.pi / (count + 1) * turns) * np.sqrt(2.0 / (count + 1))


def two_terms(table):
    high = table.astype(np.float32).astype(ml_dtypes.bfloat16)
    low = (table - high.astype(np.float64)).astype(np.float32).astype(ml_dtypes.bfloat16)
    return high, low


def tables():
    high, low = two_terms(mode_table(NX))
    pick = lambda t: t.reshape(NX, ROWS, PARTS // 2, 2, STEP).transpose(2, 0, 3, 1, 4).reshape(PARTS // 2, NX, 2 * ROWS * STEP)
    table_x = np.stack([pick(high), pick(low)], axis=1)
    high, low = two_terms(mode_table(NY))
    swap = lambda t: t.reshape(NY // 128, 128, ROWS, YL // 4, 4).transpose(0, 1, 2, 4, 3).reshape(NY // 128, 128, NY)
    table_y = np.concatenate([swap(high), swap(low)], axis=1)
    table_z = np.stack(two_terms(mode_table(NZ)))
    return table_x, table_y, table_z


def split(values):
    high = values.astype(BF16)
    return high, (values - high.astype(F32)).astype(BF16)


def dot(a, b, b_dim=0):
    return lax.dot_general(a, b, (((1,), (b_dim,)), ((), ())), preferred_element_type=F32)


def exchange_groups(values):
    lane = lax.broadcasted_iota(jnp.int32, values[0].shape, 1)
    low_half, even = lane < 64, lane % 64 < 32
    a, b, c, d = values
    a, c = jnp.where(low_half, a, pltpu.roll(c, 64, 1)), jnp.where(low_half, pltpu.roll(a, 64, 1), c)
    b, d = jnp.where(low_half, b, pltpu.roll(d, 64, 1)), jnp.where(low_half, pltpu.roll(b, 64, 1), d)
    a, b = jnp.where(even, a, pltpu.roll(b, 32, 1)), jnp.where(even, pltpu.roll(a, 96, 1), b)
    c, d = jnp.where(even, c, pltpu.roll(d, 32, 1)), jnp.where(even, pltpu.roll(c, 96, 1), d)
    return a, b, c, d


def z_transform(piece, table):
    groups = [exchange_groups([piece(g * 4 + j) for j in range(4)]) for g in range(2)]
    for pair in range(2):
        lines = [jnp.concatenate([groups[0][2 * pair + e], groups[1][2 * pair + e]], axis=1) for e in range(2)]
        high, low = split(jnp.concatenate(lines, axis=0))
        both = dot(jnp.concatenate([high, low], axis=0), table[0])
        yield both[:128] + both[128:] + dot(high, table[1])


def finish(result, tail, table, weights, mixing, out, mixed, sem):
    done = KX - 4
    copies = [pltpu.make_async_copy(result.at[a, pl.ds(0, done)], out.at[a, pl.ds(0, done)], sem.at[a]) for a in range(NF)]
    copies += [pltpu.make_async_copy(mixed.at[a], out.at[a, pl.ds(done, 4)], sem.at[NF + a]) for a in range(NF)]
    for copy in copies[:NF]:
        copy.start()
    for pair, values in enumerate(z_transform(lambda c: tail[c], table)):
        for e in range(2):
            x = 2 * pair + e
            one, two, weight = result[0, done + x], values[e * KY:(e + 1) * KY], weights[x]
            rest = 1.0 - weight
            mixed[0, x] = weight * one + rest * (mixing[0] * one + mixing[1] * two)
            mixed[1, x] = weight * two + rest * (mixing[2] * one + mixing[3] * two)
    for copy in copies[NF:]:
        copy.start()
    for copy in copies:
        copy.wait()


def kernel(
    coupling_far, sym_x_far, sym_y_far, sym_z_far, field, table_x, table_y, table_z, result, tail, tz, weights, mixing,
    coupling, sym_x, sym_y, sym_z, raw, tx, ty, turn, row_out, row_in, col_out, col_in, base,
    load_sem, row_send, row_recv, col_send, col_recv,
):
    row, col = lax.axis_index("row"), lax.axis_index("col")
    turn_of = 1 + 2 * (col % 2)
    row_peers = [(row // RX + s // RX * turn_of) % RY * RX + (row + s % RX * turn_of) % RX for s in ROW_ORDER]
    turn_of = 1 + 2 * (col % 2)
    col_peers = [(col // CC + s // CC * turn_of) % CZ * CC + (col + s % CC) % CC for s in COL_ORDER]
    last = CHUNKS - 1

    pieces = [pl.ds(n * 512, 512) for n in range(2)]
    pairs = [(table_x.at[0], tx.at[0])] + [(field.at[0, piece], raw.at[0, piece]) for piece in pieces]
    pairs += [(field.at[1], raw.at[1]), (table_x.at[1], tx.at[1])]
    pairs += [(table_y, ty), (table_z, tz), (sym_y_far, sym_y), (sym_z_far, sym_z), (sym_x_far, sym_x), (coupling_far, coupling)]
    loads = [pltpu.make_async_copy(src, dst, load_sem.at[n]) for n, (src, dst) in enumerate(pairs)]
    for load in loads[:3]:
        load.start()

    barrier = pltpu.get_barrier_semaphore()
    for peer in row_peers:
        pl.semaphore_signal(barrier, inc=1, device_id=(peer, col), device_id_type=MESH)
    for peer in col_peers:
        pl.semaphore_signal(barrier, inc=1, device_id=(row, peer), device_id_type=MESH)

    def wait_bytes(ref, sem):
        pltpu.make_async_copy(ref, ref, sem).wait()

    def make_base():
        for block in range(NY // 128):
            lanes = jnp.transpose(jnp.broadcast_to(sym_y[:, block * 128:(block + 1) * 128], (128, 128)))

            @pl.when(col // 2 == block)
            def _():
                mine = jnp.where(col % 2 == 0, lanes[0:64], lanes[64:128])
                base[...] = 1.0 + jnp.concatenate([mine, mine], axis=1) + sym_z[...]

    def row_exchange(i, kbs, sem):
        for peer in row_peers:
            pltpu.make_async_remote_copy(
                src_ref=row_out.at[i, peer, *kbs], dst_ref=row_in.at[i, row, *kbs], send_sem=row_send, recv_sem=sem,
                device_id=(peer, col), device_id_type=MESH,
            ).start()
        pltpu.make_async_copy(row_out.at[i, row, *kbs], row_in.at[i, row, *kbs], sem).start()

    def col_exchange(i, kbs, sem):
        for peer in col_peers:
            pltpu.make_async_remote_copy(
                src_ref=col_out.at[i, peer, *kbs], dst_ref=col_in.at[i, col, *kbs], send_sem=col_send, recv_sem=sem,
                device_id=(row, peer), device_id_type=MESH,
            ).start()
        pltpu.make_async_copy(col_out.at[i, col, *kbs], col_in.at[i, col, *kbs], sem).start()

    def x_step(u):
        h, a = u // 2, u % 2
        for n, when in ((0, 0), (1, 0), (2, 0), (3, 1), (4, 2)):
            pl.when(u == when)(loads[n].wait)

        @pl.when(u == 0)
        def _():
            for load in loads[3:]:
                load.start()

        def lines(n, carry):
            rows = pl.ds(pl.multiple_of(n * 128, 128), 128)
            high, low = split(raw[a, rows, :])
            both = dot(jnp.concatenate([high, low], axis=0), tx[h, 0])
            values = both[:128] + both[128:] + dot(high, tx[h, 1])
            for b in range(2):
                flipped = jnp.transpose(values[:, b * 128:(b + 1) * 128])
                for r in range(ROWS):
                    turn[b, r, pl.ds(n, 8, stride=8), :] = flipped[r * 8:(r + 1) * 8]
            return carry
        lax.fori_loop(0, YL // 4, lines, 0, unroll=8)

        for b in range(2):
            i = 2 * u + b
            for kb in range(2):
                for r in range(0, ROWS, 4):
                    parts = [turn[b, r:r + 4, (kb * 4 + k) * 8:(kb * 4 + k + 1) * 8, :].reshape(32, 128) for k in range(4)]
                    for g, part in enumerate(exchange_groups(parts)):
                        row_out[i, r:r + 4, kb, g * 8:(g + 1) * 8, :] = part.reshape(4, 8, 128)
                if b * 2 + kb < AHEAD:
                    @pl.when(u == 0)
                    def _():
                        if b == 0 and kb == 0:
                            pl.semaphore_wait(barrier, ROWS + COLS - 2)
                        row_exchange(i, (kb,), row_recv.at[i, kb])

    def y_step(i, kb, count):
        kbs = pl.ds(kb, count)
        wait_bytes(row_in.at[i, :, kbs], row_recv.at[i, kb])
        lines = jnp.concatenate([row_in[i, :, kb + k].reshape(NY, 128) for k in range(count)], axis=1)
        high, low = split(lines)
        terms = jnp.concatenate([high, low], axis=1)
        for m in range(NY // 128):
            four = dot(ty[m], terms)
            values = four[:128, :128] + (four[128:, :128] + four[:128, 128:])
            col_out[i, 2 * m:2 * m + 2, kb] = values.reshape(2, KY, 128)
        col_exchange(i, (kb,), col_recv.at[i, kb])

    def z_wait(i, kb, count):
        wait_bytes(col_in.at[i, :, pl.ds(kb, count)], col_recv.at[i, kb])

    def z_step(i, kb, count):
        a, first_x = i // 2 % 2, (i // 4 * 2 + i % 2) * STEP + kb * 4
        for k in range(count):
            for pair, values in enumerate(z_transform(lambda c: col_in[i, c, kb + k], tz)):
                result[a, pl.ds(first_x + k * 4 + 2 * pair, 2)] = values.reshape(2, KY, NZ)

        @pl.when(a == 1)
        def _():
            def mix(n, carry):
                x = first_x + n
                one, two = result[0, x], result[1, x]
                weight = 1.0 / (base[...] + sym_x[row * KX + x])
                rest = 1.0 - weight
                result[0, x] = weight * one + rest * (coupling[0, 0] * one + coupling[0, 1] * two)
                result[1, x] = weight * two + rest * (coupling[1, 0] * one + coupling[1, 1] * two)
                return carry
            lax.fori_loop(0, 4 * count, mix, 0, unroll=4)

    def halves(step):
        def body(kb, carry):
            step(kb)
            return carry
        lax.fori_loop(0, 2, body, 0)

    lag = LAG_Z

    def send(j):
        @pl.when(j < 2 * CHUNKS)
        def _():
            row_exchange(j // 2, (j % 2,), row_recv.at[j // 2, j % 2])

    def middle(j, carry):
        pl.when(jnp.logical_or(j == 2, j == 6))(lambda: x_step((j + 6) // 4))
        send(j + AHEAD)
        y_step(j // 2, j % 2, 1)

        @pl.when(j >= lag)
        def _():
            z_wait((j - lag) // 2, (j - lag) % 2, 1)
            z_step((j - lag) // 2, (j - lag) % 2, 1)
        return carry

    halves(x_step)
    for load in loads[5:]:
        load.wait()
    make_base()
    for x in range(4):
        weights[x] = 1.0 / (base[...] + sym_x[row * KX + KX - 4 + x])
    for n in range(NF * NF):
        mixing[n] = jnp.full((KY, NZ), coupling[n // NF, n % NF], F32)
    lax.fori_loop(0, 2 * CHUNKS, middle, 0)

    def final(j, carry):
        z_wait(j // 2, j % 2, 1)
        z_step(j // 2, j % 2, 1)
        return carry
    lax.fori_loop(2 * CHUNKS - lag, 2 * CHUNKS - 1, final, 0)
    z_wait(last, 1, 1)
    tail[...] = col_in[last, :, 1]
    wait_bytes(row_out.at[:, pl.ds(0, ROWS - 1)], row_send)
    wait_bytes(col_out.at[:, pl.ds(0, COLS - 1)], col_send)


def local(species, coupling, symbol_x, symbol_y, symbol_z):
    field = jnp.transpose(species, (0, 2, 3, 1)).reshape(NF, YL * ZL, NX)
    operands = (coupling, symbol_x, symbol_y.reshape(1, NY), symbol_z.reshape(1, NZ), field, *map(jnp.asarray, tables()))
    far = pl.BlockSpec(memory_space=pltpu.HBM)
    parts = pl.pallas_call(
        kernel,
        out_shape=[
            pltpu.VMEM((NF, KX, KY, NZ), F32),
            pltpu.VMEM((COLS, KY, 128), F32),
            pltpu.VMEM((2, NZ, NZ), BF16),
            pltpu.VMEM((4, KY, NZ), F32),
            pltpu.VMEM((NF * NF, KY, NZ), F32),
        ],
        in_specs=[far] * 8,
        out_specs=[pl.BlockSpec(memory_space=pltpu.VMEM)] * 5,
        scratch_shapes=[
            pltpu.SMEM((NF, NF), F32),
            pltpu.SMEM((NX,), F32),
            pltpu.VMEM((1, NY), F32),
            pltpu.VMEM((1, NZ), F32),
            pltpu.VMEM((NF, YL * ZL, NX), F32),
            pltpu.VMEM((PARTS // 2, 2, NX, 2 * ROWS * STEP), BF16),
            pltpu.VMEM((NY // 128, 256, NY), BF16),
            pltpu.VMEM((2, ROWS, 72, 128), F32),
            pltpu.VMEM((CHUNKS, ROWS, 2, YL, 128), F32),
            pltpu.VMEM((CHUNKS, ROWS, 2, YL, 128), F32),
            pltpu.VMEM((CHUNKS, COLS, 2, KY, 128), F32),
            pltpu.VMEM((CHUNKS, COLS, 2, KY, 128), F32),
            pltpu.VMEM((KY, NZ), F32),
            pltpu.SemaphoreType.DMA((11,)),
            pltpu.SemaphoreType.DMA,
            pltpu.SemaphoreType.DMA((CHUNKS, 2)),
            pltpu.SemaphoreType.DMA,
            pltpu.SemaphoreType.DMA((CHUNKS, 2)),
        ],
        compiler_params=pltpu.CompilerParams(collective_id=1, has_side_effects=True, vmem_limit_bytes=40 << 20),
        name="sine_modes",
    )(*(pltpu.with_memory_space_constraint(operand, pltpu.HBM) for operand in operands))
    return pl.pallas_call(
        finish,
        out_shape=pltpu.HBM((NF, KX, KY, NZ), F32),
        in_specs=[pl.BlockSpec(memory_space=pltpu.VMEM)] * 5,
        out_specs=far,
        scratch_shapes=[pltpu.VMEM((NF, 4, KY, NZ), F32), pltpu.SemaphoreType.DMA((2 * NF,))],
        compiler_params=pltpu.CompilerParams(vmem_limit_bytes=8 << 20),
        name="finish",
    )(*(pltpu.with_memory_space_constraint(part, pltpu.VMEM) for part in parts))


def solution(mesh):
    return jax.shard_map(
        local,
        mesh=mesh,
        in_specs=(P(None, None, "row", "col"), P(), P(), P(), P()),
        out_specs=P(None, "row", "col", None),
        check_vma=False,
    )
```
